32 devices in a mesh: dp: 4 (over y, core), fsdp: 8 (over z, x).
Axes of the slice: x: 2, y: 2, z: 4, core: 2. Of those that a mesh axis runs over, the one named last changes fastest.
Arguments:
- inputs: bfloat16 [4, 2, 1024, 2048], P('dp', None, 'fsdp'), may hold values from -6 to 6
- norm_gain: bfloat16 [2, 2048], replicated, may hold values from 0.5 to 1.5
- norm_bias: bfloat16 [2, 2048], replicated, may hold values from -1.75 to 1.75
- w_qkv: bfloat16 [2048, 6144], P(None, 'fsdp'), may hold values from -0.125 to 0.125
- qv_bias: bfloat16 [2, 2048], replicated, may hold values from -0.625 to 0.625
- w_out: bfloat16 [2048, 2048], P(None, 'fsdp'), may hold values from -0.5 to 0.5
- out_bias: bfloat16 [2048], replicated, may hold values from -1.75 to 1.75
- w_up: bfloat16 [2048, 8192], P(None, 'fsdp'), may hold values from -0.125 to 0.125
- up_bias: bfloat16 [8192], replicated, may hold values from -3 to 3
- w_down: bfloat16 [8192, 2048], P(None, 'fsdp'), may hold values from -0.0625 to 0.0625
- down_bias: bfloat16 [2048], replicated, may hold values from -1.75 to 1.75
- adapter_index: int32 [8], replicated, may hold values from 0 to 7
- ad_in_qkv: bfloat16 [8, 2048, 48], replicated, may hold values from -0.125 to 0.125
- ad_out_qkv: bfloat16 [8, 3, 16, 2048], replicated, may hold values from -0.75 to 0.75
- ad_in_out: bfloat16 [8, 2048, 16], replicated, may hold values from -0.5 to 0.5
- ad_out_out: bfloat16 [8, 16, 2048], replicated, may hold values from -0.75 to 0.75
- ad_in_up: bfloat16 [8, 2048, 16], replicated, may hold values from -0.125 to 0.125
- ad_out_up: bfloat16 [8, 16, 8192], replicated, may hold values from -0.75 to 0.75
- ad_in_down: bfloat16 [8, 8192, 16], replicated, may hold values from -0.0625 to 0.0625
- ad_out_down: bfloat16 [8, 16, 2048], replicated, may hold values from -0.75 to 0.75
- cotangent: bfloat16 [4, 2, 1024, 2048], P('dp', None, 'fsdp'), may hold values from -6 to 6
Outputs:
- outputs: bfloat16 [4, 2, 1024, 2048], P('dp', None, 'fsdp')
- input_grad: float32 [4, 2, 1024, 2048], P('dp', None, 'fsdp')
- grad_in_qkv: float32 [8, 2048, 48], replicated
- grad_out_qkv: float32 [8, 3, 16, 2048], replicated
- grad_in_out: float32 [8, 2048, 16], replicated
- grad_out_out: float32 [8, 16, 2048], replicated
- grad_in_up: float32 [8, 2048, 16], replicated
- grad_out_up: float32 [8, 16, 8192], replicated
- grad_in_down: float32 [8, 8192, 16], replicated
- grad_out_down: float32 [8, 16, 2048], replicated
The draws below stay inside these ranges and needn't reach their ends.
Inputs may be any that keep to these rules, and one draw needn't show every extreme that they name: adapter_index[s] names the adapter of sequence s.
All inputs are finite; a program needn't handle non-finite values.
Results may differ from the reference program's by a relative error of at most 0.014.
Values may be sent and summed in bfloat16 or wider, within the bound.
A program may use at most 448 MiB of HBM per device.

```python
import jax
import jax.numpy as jnp
from jax import lax

D = 2048
H = 16
HD = 128
FF = 8192
R = 16
NA = 8
MB = 2
TOKENS_MB = 1024
SEQ = 1024
NSEQ = 8
N_DP = 4


def plant(values, key, smallest, top_value):
    longest = values.shape.index(max(values.shape))
    spots = []
    for shift in (0, 1):
        where = [jax.random.randint(jax.random.fold_in(key, axis), (), 0, length) for axis, length in enumerate(values.shape)]
        where[longest] = (where[longest] + shift) % values.shape[longest]
        spots.append(tuple(where))
    return values.at[spots[0]].set(smallest).at[spots[1]].set(top_value)


def level_of(key, shape, cuts, smallest, largest):
    level, own = 1.0, jax.random.fold_in(key, 6)
    for axis_at, parts in cuts:
        heights = jnp.exp(jax.random.uniform(jax.random.fold_in(own, axis_at), (parts,), jnp.float32, smallest / len(cuts), largest / len(cuts)))
        level = level * jnp.repeat(heights, shape[axis_at] // parts).reshape([-1 if axis == axis_at else 1 for axis in range(len(shape))])
    return level


def scatter_about(stream_key, extent, scale, most, shards=(), kind=jnp.bfloat16):
    entries = jax.random.normal(stream_key, extent, jnp.float32) * scale
    if len(shards) > 0:
        entries = level_of(stream_key, extent, shards, -0.22, 0.18) * entries
    return jnp.clip(entries, min=-most, max=most).astype(kind)


def setup_inputs(seed: int = 0) -> dict:
    key_list = jax.random.split(jax.random.key(seed), 22)
    inputs = scatter_about(key_list[0], (N_DP, MB, TOKENS_MB, D), 1.0, 6.0, ((0, 4), (2, 8)))
    norm_gain = jnp.clip(1.0 + 0.1 * jax.random.normal(key_list[1], (2, D), jnp.float32), 0.5, 1.5).astype(jnp.bfloat16)
    norm_bias = scatter_about(key_list[2], (2, D), 0.3, 1.75)
    w_qkv = scatter_about(key_list[3], (D, 3 * D), D ** -0.5, 0.125, ((1, 8),))
    qv_bias = scatter_about(key_list[4], (2, D), 0.1, 0.625)
    w_out = scatter_about(key_list[5], (D, D), (D // 16) ** -0.5, 0.5, ((1, 8),))
    out_bias = scatter_about(key_list[6], (D,), 0.3, 1.75)
    w_up = scatter_about(key_list[7], (D, FF), D ** -0.5, 0.125, ((1, 8),))
    up_bias = scatter_about(key_list[8], (FF,), 0.5, 3.0)
    w_down = scatter_about(key_list[9], (FF, D), FF ** -0.5, 0.0625, ((1, 8),))
    down_bias = scatter_about(key_list[10], (D,), 0.3, 1.75)
    adapter_index = plant(jax.random.randint(key_list[11], (NSEQ,), 0, NA), jax.random.fold_in(key_list[11], 1), 0, NA - 1).astype(jnp.int32)
    ad_in_qkv = scatter_about(key_list[12], (NA, D, 3 * R), D ** -0.5, 0.125)
    ad_out_qkv = scatter_about(key_list[13], (NA, 3, R, D), (4 * R) ** -0.5, 0.75)
    ad_in_out = scatter_about(key_list[14], (NA, D, R), (D // 16) ** -0.5, 0.5)
    ad_out_out = scatter_about(key_list[15], (NA, R, D), (4 * R) ** -0.5, 0.75)
    ad_in_up = scatter_about(key_list[16], (NA, D, R), D ** -0.5, 0.125)
    ad_out_up = scatter_about(key_list[17], (NA, R, FF), (4 * R) ** -0.5, 0.75)
    ad_in_down = scatter_about(key_list[18], (NA, FF, R), FF ** -0.5, 0.0625)
    ad_out_down = scatter_about(key_list[19], (NA, R, D), (4 * R) ** -0.5, 0.75)
    cotangent = scatter_about(key_list[20], (N_DP, MB, TOKENS_MB, D), 1.0, 6.0, ((0, 4), (2, 8)))
    return dict(inputs=inputs, norm_gain=norm_gain, norm_bias=norm_bias, w_qkv=w_qkv, qv_bias=qv_bias, w_out=w_out, out_bias=out_bias, w_up=w_up, up_bias=up_bias, w_down=w_down, down_bias=down_bias, adapter_index=adapter_index, ad_in_qkv=ad_in_qkv, ad_out_qkv=ad_out_qkv, ad_in_out=ad_in_out, ad_out_out=ad_out_out, ad_in_up=ad_in_up, ad_out_up=ad_out_up, ad_in_down=ad_in_down, ad_out_down=ad_out_down, cotangent=cotangent)


@jax.custom_vjp
def low(v):
    return lax.optimization_barrier(v.astype(jnp.bfloat16)).astype(jnp.float32)

@jax.custom_vjp
def low_back(v):
    return v

def low_keep(v):
    return (low(v), None)

def low_pass(kept, grad):
    return (grad,)

def back_keep(v):
    return (v, None)

def back_low(kept, grad):
    return (low(grad),)
low.defvjp(low_keep, low_pass)
low_back.defvjp(back_keep, back_low)
epsilon = 1e-05
masked_fill = -1e+30

def matmul(left_side, right_side):
    return jnp.dot(left_side, right_side, precision=lax.Precision.HIGHEST, preferred_element_type=jnp.float32)

def normalize(values, gain_row, shift_row):
    centred = values - lax.optimization_barrier(jnp.mean(values, -1, keepdims=True))
    spread = lax.optimization_barrier(jnp.mean(centred * centred, -1, keepdims=True))
    return centred * lax.rsqrt(spread + epsilon) * gain_row + shift_row

def attend(queries, keys_all, values_all):
    length = queries.shape[0]
    causal = jnp.arange(length)[:, None] >= jnp.arange(length)[None, :]
    score_scale = HD ** (-0.5)

    def one_head(operands):
        query_head, key_head, value_head = operands
        scores = low_back(matmul(query_head, key_head.T) * score_scale)
        scores = jnp.where(causal, scores, masked_fill)
        weights = low(jax.nn.softmax(scores, axis=-1))
        return matmul(weights, value_head)

    def to_heads(values):
        return values.reshape(length, H, HD).transpose(1, 0, 2)
    mixed = lax.map(jax.checkpoint(one_head), (to_heads(queries), to_heads(keys_all), to_heads(values_all)))
    return mixed.transpose(1, 0, 2).reshape(length, H * HD)

def layer(values, tables, adapter_id, frozen):
    gains, shifts, w_qkv, qv_bias, w_out, out_bias, w_up, up_bias, w_down, down_bias = frozen
    in_qkv, out_qkv, in_out, out_out, in_up, out_up, in_down, out_down = [table_all[adapter_id] for table_all in tables]
    first_norm = low(normalize(values, gains[0], shifts[0]))
    low_qkv = low(low_back(matmul(first_norm, in_qkv)))
    base_qkv = matmul(first_norm, w_qkv)
    queries = base_qkv[:, 0:D] + qv_bias[0] + matmul(low_qkv[:, 0:R], out_qkv[0])
    keys_all = base_qkv[:, D:2 * D] + matmul(low_qkv[:, R:2 * R], out_qkv[1])
    values_all = base_qkv[:, 2 * D:3 * D] + qv_bias[1] + matmul(low_qkv[:, 2 * R:3 * R], out_qkv[2])
    queries = low(low_back(queries))
    keys_all = low(low_back(keys_all))
    values_all = low(low_back(values_all))
    context = low(low_back(attend(queries, keys_all, values_all)))
    low_out = low(low_back(matmul(context, in_out)))
    attn = low_back(matmul(context, w_out) + out_bias + matmul(low_out, out_out))
    middle = values + attn
    second_norm = low(normalize(middle, gains[1], shifts[1]))
    low_up = low(low_back(matmul(second_norm, in_up)))
    pre_act = low_back(matmul(second_norm, w_up) + up_bias + matmul(low_up, out_up))
    activated = low(jax.nn.gelu(pre_act, approximate=False))
    low_down = low(low_back(matmul(activated, in_down)))
    ffn_out = low_back(matmul(activated, w_down) + down_bias + matmul(low_down, out_down))
    return middle + ffn_out

def reference(inputs, norm_gain, norm_bias, w_qkv, qv_bias, w_out, out_bias, w_up, up_bias, w_down, down_bias, adapter_index, ad_in_qkv, ad_out_qkv, ad_in_out, ad_out_out, ad_in_up, ad_out_up, ad_in_down, ad_out_down, cotangent):
    frozen = tuple((member_array.astype(jnp.float32) for member_array in (norm_gain, norm_bias, w_qkv, qv_bias, w_out, out_bias, w_up, up_bias, w_down, down_bias)))
    tables = tuple((member_array.astype(jnp.float32) for member_array in (ad_in_qkv, ad_out_qkv, ad_in_out, ad_out_out, ad_in_up, ad_out_up, ad_in_down, ad_out_down)))
    sequences = inputs.astype(jnp.float32).reshape(NSEQ, SEQ, D)
    tangents = cotangent.astype(jnp.float32).reshape(NSEQ, SEQ, D)

    def one_sequence(running, operands):
        values, tangent, adapter_id = operands
        result, pull_back = jax.vjp(lambda row_values, table_values: layer(row_values, table_values, adapter_id, frozen), values, tables)
        grad_values, grad_tables = pull_back(tangent)
        updated = tuple((partial_sum + addend for partial_sum, addend in zip(running, grad_tables)))
        return (updated, (result, grad_values))
    initial = tuple((jnp.zeros_like(member_array) for member_array in tables))
    totals, (results, grads_all) = lax.scan(one_sequence, initial, (sequences, tangents, adapter_index))
    out_shape = (N_DP, MB, TOKENS_MB, D)
    return (results.astype(jnp.bfloat16).reshape(out_shape), grads_all.reshape(out_shape), totals[0], totals[1], totals[2], totals[3], totals[4], totals[5], totals[6], totals[7])
```

```python
import functools

import jax
import jax.numpy as jnp
from jax import lax
from jax.experimental import pallas as pl
from jax.experimental.pallas import tpu as pltpu
from jax.sharding import Mesh
from jax.sharding import PartitionSpec as P

H = 16
EPS = 1e-05
MASKED = -1e30
F32 = jnp.float32
BF16 = jnp.bfloat16
PAD = 128


def nn(a, b):
    return jnp.dot(a, b, preferred_element_type=F32)


def nt(a, b):
    return lax.dot_general(a, b, (((1,), (1,)), ((), ())), preferred_element_type=F32)


def tn(a, b):
    return lax.dot_general(a, b, (((0,), (0,)), ((), ())), preferred_element_type=F32)


def centre(v):
    c = v - jnp.mean(v, -1, keepdims=True)
    rstd = lax.rsqrt(jnp.mean(c * c, -1, keepdims=True) + EPS)
    return c * rstd, rstd


def norm_back(v, grad, gain):
    nh, rstd = centre(v)
    e = gain * grad
    return rstd * (e - jnp.mean(e, -1, keepdims=True) - nh * jnp.mean(nh * e, -1, keepdims=True))


def full(shape):
    return pl.BlockSpec(shape, lambda *_: (0,) * len(shape))


def once(shape):
    return pl.BlockSpec(shape, lambda *_: (0,) * len(shape), pipeline_mode=pl.Buffered(1))


def rows(tile, width):
    return pl.BlockSpec((tile, width), lambda i: (i, 0))


def cols(height, tile):
    return pl.BlockSpec((height, tile), lambda i: (0, i))


def call(body, grid, ins, outs, name, flops=0, size=0, scratch=()):
    arrays = [a for a, _ in ins]
    return pl.pallas_call(
        body,
        grid=grid,
        in_specs=[s for _, s in ins],
        out_specs=[s for _, s in outs],
        out_shape=[a for a, _ in outs],
        scratch_shapes=list(scratch),
        cost_estimate=pl.CostEstimate(flops=flops, bytes_accessed=size, transcendentals=0),
        name=name,
    )(*arrays)


def sds(shape, dtype=BF16):
    return jax.ShapeDtypeStruct(shape, dtype)


def row_loop(count, tile, step):
    @pl.loop(0, count // tile)
    def _(r):
        step(pl.ds(pl.multiple_of(r * tile, tile), tile))


def norm_kernel(x_ref, gain_ref, shift_ref, out_ref):
    nh, _ = centre(x_ref[...].astype(F32))
    out_ref[...] = (nh * gain_ref[...] + shift_ref[...]).astype(BF16)


def mid_kernel(x_ref, a_ref, b_ref, bias_ref, low_ref, gain_ref, shift_ref, mid_ref, h_ref, lo_ref):
    d = x_ref.shape[1]
    r = low_ref.shape[0]
    s = a_ref[...].astype(F32) + b_ref[...].astype(F32)
    lo = s[:, d : d + PAD][:, :r].astype(BF16)
    lo_ref[...] = lo
    mid = x_ref[...].astype(F32) + s[:, :d] + bias_ref[...] + nn(lo, low_ref[...])
    mid_ref[...] = mid
    nh, _ = centre(mid)
    h_ref[...] = (nh * gain_ref[...] + shift_ref[...]).astype(BF16)


def out_kernel(mid_ref, a_ref, b_ref, bias_ref, low_ref, g_ref, out_ref, term_ref):
    d = mid_ref.shape[1]
    r = low_ref.shape[0]
    s = a_ref[...].astype(F32) + b_ref[...].astype(F32)
    ld = s[:, d : d + PAD][:, :r].astype(BF16)
    out_ref[...] = (mid_ref[...] + s[:, :d] + bias_ref[...] + nn(ld, low_ref[...])).astype(BF16)
    term = tn(ld, g_ref[...])

    @pl.when(pl.program_id(0) == 0)
    def _():
        term_ref[...] = term

    @pl.when(pl.program_id(0) > 0)
    def _():
        term_ref[...] += term


def gmid_kernel(mid_ref, g_ref, a_ref, b_ref, low_ref, gain_ref, h_ref, lo_ref, gmid_ref, gattn_ref, tin_ref, tout_ref):
    d = mid_ref.shape[1]
    r = low_ref.shape[0]
    s = a_ref[...].astype(F32) + b_ref[...].astype(F32)
    glu = s[:, d : d + PAD][:, :r].astype(BF16)
    gh = s[:, :d] + nn(glu, low_ref[...])
    gmid = g_ref[...].astype(F32) + norm_back(mid_ref[...], gh, gain_ref[...])
    gmid_ref[...] = gmid
    gattn = gmid.astype(BF16)
    gattn_ref[...] = gattn
    tin = tn(glu, h_ref[...])
    tout = tn(lo_ref[...], gattn)

    @pl.when(pl.program_id(0) == 0)
    def _():
        tin_ref[...] = tin
        tout_ref[...] = tout

    @pl.when(pl.program_id(0) > 0)
    def _():
        tin_ref[...] += tin
        tout_ref[...] += tout


def final_kernel(x_ref, gmid_ref, a_ref, b_ref, low_ref, gain_ref, h_ref, out_ref, tin_ref):
    d = x_ref.shape[1]
    r = low_ref.shape[0]
    s = a_ref[...].astype(F32) + b_ref[...].astype(F32)
    glq = s[:, d : d + PAD][:, :r].astype(BF16)
    gh = s[:, :d] + nn(glq, low_ref[...])
    out_ref[...] = (gmid_ref[...] + norm_back(x_ref[...].astype(F32), gh, gain_ref[...])).astype(BF16)
    tin = tn(glq, h_ref[...])

    @pl.when(pl.program_id(0) == 0)
    def _():
        tin_ref[...] = tin

    @pl.when(pl.program_id(0) > 0)
    def _():
        tin_ref[...] += tin


def qkv_kernel(tile, h_ref, w_ref, in_ref, ao_ref, bias_ref, out_ref, lq_ref):
    first = pl.program_id(0) == 0

    def step(at):
        @pl.when(first)
        def _():
            lq_ref[at, :] = nt(h_ref[at, :], in_ref[...]).astype(BF16)

        acc = nn(h_ref[at, :], w_ref[0]) + nn(lq_ref[at, :], ao_ref[...])
        out_ref[at, :] = (acc + bias_ref[...]).astype(BF16)

    row_loop(h_ref.shape[0], tile, step)


def up_kernel(tile, h_ref, w_ref, in_ref, ao_ref, bias_ref, act_ref, slope_ref, lu_ref):
    first = pl.program_id(0) == 0

    def step(at):
        @pl.when(first)
        def _():
            lu_ref[at, :] = nt(h_ref[at, :], in_ref[...]).astype(BF16)

        pre = nn(h_ref[at, :], w_ref[0]) + nn(lu_ref[at, :], ao_ref[...]) + bias_ref[...]
        cdf = 0.5 * (1.0 + lax.erf(pre * (0.5**0.5)))
        pdf = jnp.exp(-0.5 * pre * pre) * 0.3989422804014327
        act_ref[at, :] = (pre * cdf).astype(BF16)
        slope_ref[at, :] = (cdf + pre * pdf).astype(BF16)

    row_loop(h_ref.shape[0], tile, step)


def down_kernel(tile, width, a_ref, w_ref, low_ref, out_ref):
    i = pl.program_id(0)
    nc = w_ref.shape[2]

    def step(at):
        out_ref[at, pl.ds(pl.multiple_of(i * nc, nc), nc)] = nn(a_ref[at, :], w_ref[0]).astype(BF16)

        @pl.when(i == 0)
        def _():
            low = nt(a_ref[at, :], low_ref[...])
            pad = jnp.zeros((tile, PAD - low.shape[1]), F32)
            out_ref[at, pl.ds(width, PAD)] = jnp.concatenate([low, pad], 1).astype(BF16)

    row_loop(a_ref.shape[0], tile, step)


def gpre_kernel(tile, g_ref, w_ref, slope_ref, act_ref, outlow_ref, inlow_ref, lu_ref, gpre_ref, gld_ref, tin_ref, tout_ref):
    first = pl.program_id(0) == 0
    parts, nc = w_ref.shape[0], w_ref.shape[2]

    def step(at):
        @pl.when(first)
        def _():
            gld_ref[at, :] = nt(g_ref[at, :], outlow_ref[...]).astype(BF16)

        acc = nn(gld_ref[at, :], inlow_ref[...])
        for p in range(parts):
            acc += nt(g_ref[at, p * nc : (p + 1) * nc], w_ref[p])
        gpre_ref[at, :] = (acc * slope_ref[at, :].astype(F32)).astype(BF16)

    row_loop(g_ref.shape[0], tile, step)
    tin_ref[...] = tn(gld_ref[...], act_ref[...]).astype(BF16)
    tout_ref[...] = tn(lu_ref[...], gpre_ref[...]).astype(BF16)


def back_kernel(tile, width, g_ref, w_ref, low_ref, out_ref):
    i = pl.program_id(0)
    parts, dt, nc = w_ref.shape

    def step(at):
        acc = nt(g_ref[at, 0:nc], w_ref[0])
        for p in range(1, parts):
            acc += nt(g_ref[at, p * nc : (p + 1) * nc], w_ref[p])
        out_ref[at, pl.ds(pl.multiple_of(i * dt, dt), dt)] = acc.astype(BF16)

        @pl.when(i == 0)
        def _():
            low = nt(g_ref[at, :], low_ref[...])
            pad = jnp.zeros((tile, PAD - low.shape[1]), F32)
            out_ref[at, pl.ds(width, PAD)] = jnp.concatenate([low, pad], 1).astype(BF16)

    row_loop(g_ref.shape[0], tile, step)


def gctx_kernel(tile, g_ref, w_ref, outlow_ref, inlow_ref, ctx_ref, gctx_ref, term_ref, glo_ref):
    parts, nc = w_ref.shape[0], w_ref.shape[2]

    def step(at):
        glo = nt(g_ref[at, :], outlow_ref[...]).astype(BF16)
        glo_ref[at, :] = glo
        acc = nn(glo, inlow_ref[...])
        for p in range(parts):
            acc += nt(g_ref[at, p * nc : (p + 1) * nc], w_ref[p])
        gctx_ref[at, :] = acc.astype(BF16)

    row_loop(g_ref.shape[0], tile, step)
    term_ref[...] = tn(glo_ref[...], ctx_ref[...]).astype(BF16)


def softmax_block(q, k, start, scale):
    s = nt(q, k) * scale
    r = lax.broadcasted_iota(jnp.int32, s.shape, 0) + start
    c = lax.broadcasted_iota(jnp.int32, s.shape, 1)
    s = jnp.where(r >= c, s, MASKED)
    p = jnp.exp(s - jnp.max(s, -1, keepdims=True))
    return p * (1.0 / jnp.sum(p, -1, keepdims=True))


def attend_kernel(bq, scale, q_ref, k_ref, v_ref, ctx_ref):
    length = q_ref.shape[0]
    for start in range(0, length, bq):
        end = start + bq
        p = softmax_block(q_ref[start:end, :], k_ref[:end, :], start, scale)
        ctx_ref[start:end, :] = nn(p.astype(BF16), v_ref[:end, :]).astype(BF16)


def attend_back_kernel(bq, scale, q_ref, k_ref, v_ref, g_ref, lq_ref, gq_ref, gk_ref, gv_ref, tq_ref, tk_ref, tv_ref, ks, vs):
    length = q_ref.shape[0]
    r = tq_ref.shape[0]
    for start in reversed(range(0, length, bq)):
        end = start + bq
        q, g = q_ref[start:end, :], g_ref[start:end, :]
        p = softmax_block(q, k_ref[:end, :], start, scale)
        dp = nt(g, v_ref[:end, :])
        ds = (p * (dp - jnp.sum(p * dp, -1, keepdims=True))).astype(BF16)
        gq_ref[start:end, :] = (nn(ds, k_ref[:end, :]) * scale).astype(BF16)
        dk, dv = tn(ds, q), tn(p.astype(BF16), g)
        if end == length:
            ks[...] = dk
            vs[...] = dv
        else:
            ks[:end, :] += dk
            vs[:end, :] += dv
    gk_ref[...] = (ks[...] * scale).astype(BF16)
    gv_ref[...] = vs[...].astype(BF16)
    tq_ref[...] = tn(lq_ref[:, :r], gq_ref[...]).astype(BF16)
    tk_ref[...] = tn(lq_ref[:, r : 2 * r], gk_ref[...]).astype(BF16)
    tv_ref[...] = tn(lq_ref[:, 2 * r : 3 * r], gv_ref[...]).astype(BF16)


def shards(
    inputs,
    norm_gain,
    norm_bias,
    w_qkv,
    qv_bias,
    w_out,
    out_bias,
    w_up,
    up_bias,
    w_down,
    down_bias,
    adapter_index,
    ad_in_qkv,
    ad_out_qkv,
    ad_in_out,
    ad_out_out,
    ad_in_up,
    ad_out_up,
    ad_in_down,
    ad_out_down,
    cotangent,
):
    y, c, z, x = (lax.axis_index(a) for a in ("y", "c", "z", "x"))
    ny, n, nx = lax.axis_size("y"), lax.axis_size("z"), lax.axis_size("x")
    group = 2 * nx
    mb, tok, d = inputs.shape[1:]
    r = ad_out_out.shape[1]
    na = ad_in_qkv.shape[0]
    hd = d // H
    heads = H // group
    dl = d // group
    ff = up_bias.shape[0]
    fl = ff // group
    seqs = adapter_index.shape[0]
    length = 2 * ny * mb * n * nx * tok // seqs
    blocks = length // tok
    zb = blocks // nx
    per = n // zb
    own = length // group
    wide = d + PAD
    scale = hd**-0.5
    assert zb == 4 and n == 2 * mb * per and mb == 2

    def swap(v, axis):
        return lax.ppermute(v, axis, [(0, 1), (1, 0)])

    routes = []
    for odd in range(2):
        route = []
        for cs in range(2):
            for zs in range(n):
                h, zz = divmod(zs, zb)
                m = (zz + odd) % 2
                route.append((cs * n + zs, (zz // 2) * n + (cs * mb + m) * per + h))
        routes.append(route)
    slot_here = (z % zb) % 2
    m_here = (z // per) % mb

    def pick(index, pair):
        return jnp.where(index == 0, pair[0], pair[1])

    def deal(v):
        v = v[0]
        sent = [pick((slot_here + odd) % 2, (v[0], v[1])) for odd in range(2)]
        got = [lax.ppermute(s, ("c", "z"), route) for s, route in zip(sent, routes)]
        return jnp.concatenate([pick(m_here, got), pick(1 - m_here, got)], 0)

    def undeal(v):
        v = (v[:tok], v[tok:])
        sent = [pick((m_here + odd) % 2, v) for odd in range(2)]
        back = [[(b, a) for a, b in route] for route in routes]
        got = [lax.ppermute(s, ("c", "z"), route) for s, route in zip(sent, back)]
        return jnp.stack([pick(slot_here, got), pick(1 - slot_here, got)])[None]

    def spread(v):
        v = v.reshape(2, tok, v.shape[-1])
        if nx == 2:
            other = swap(v, "x")
            v = jnp.stack([pick(x, (v, other)), pick(1 - x, (v, other))], 1)
        else:
            v = lax.all_gather(v, "x", axis=1)
        other = swap(v, "c")
        v = jnp.stack([pick(c, (v, other)), pick(1 - c, (v, other))])
        return v.reshape(length, v.shape[-1])

    def half_at(v, axis, index):
        return lax.dynamic_index_in_dim(v, index, axis, keepdims=False)

    def gather_sum(v):
        w = v.shape[-1]
        v = v.reshape(2, 2 * nx * tok, w)
        got = swap(half_at(v, 0, 1 - c), "c")
        v = (half_at(v, 0, c).astype(F32) + got.astype(F32)).astype(BF16).reshape(2, nx, tok, w)
        if nx > 2:
            v = lax.psum_scatter(v.astype(F32), "x", scatter_dimension=1).astype(BF16).reshape(own, w)
            return v, jnp.zeros_like(v)
        got = swap(half_at(v, 1, 1 - x), "x")
        return half_at(v, 1, x).reshape(own, w), got.reshape(own, w)

    def collect(piece):
        k, nc = piece.shape
        half = half_at(piece.reshape(ny, k // ny, nc), 0, y)
        up = down = half
        ups, downs = [], []
        for _ in range(1, n):
            up = lax.ppermute(up, "z", [(i, i + 1) for i in range(n - 1)])
            down = lax.ppermute(down, "z", [(i + 1, i) for i in range(n - 1)])
            ups.append(up)
            downs.append(down)
        out = jnp.zeros((n, ny, k // ny, nc), piece.dtype)
        out = lax.dynamic_update_slice(out, piece.reshape(1, ny, k // ny, nc), (z, 0, 0, 0))
        for t in range(1, n):
            got = jnp.where(z + t < n, downs[t - 1], ups[n - t - 1])
            other = swap(got, "y")
            at = (z + t) % n
            out = lax.dynamic_update_slice(out, got[None, None], (at, y, 0, 0))
            out = lax.dynamic_update_slice(out, other[None, None], (at, 1 - y, 0, 0))
        return out.reshape(n, k, nc)

    def part(v, shape, lead):
        v = v.reshape(v.shape[:lead] + shape + v.shape[lead + 1 :])
        v = half_at(v, lead + 1, x)
        return half_at(v, lead + 1, c)

    ff_shape, head_shape = (n, nx, 2, fl // n), (heads, nx, 2, hd)

    def my_ff(v, axis):
        w = part(v, ff_shape, axis)
        return w.reshape(w.shape[:axis] + (fl,) + w.shape[axis + 2 :])

    def my_heads(v, axis):
        w = part(v, head_shape, axis)
        return w.reshape(w.shape[:axis] + (dl,) + w.shape[axis + 2 :])

    qcols = w_qkv.shape[1] // hd
    if nx == 2 and qcols == 6:
        wq = w_qkv.reshape(d, qcols, hd)
        k0, k1, sent = (half_at(wq, 1, c + 2 * i) for i in (0, 2, 1))
        got = swap(sent, "x")
        wq = jnp.concatenate([pick(x, (k0, got)), pick(x, (k1, k0)), pick(x, (got, k1))], 1)
        wq = collect(wq)
    else:
        wq = lax.all_gather(w_qkv, ("z", "x"), axis=1, tiled=True)
        wq = part(wq.reshape(d, 3, d), head_shape, 2).reshape(1, d, 3 * dl)

    def across(w, shape):
        w = w.reshape(shape + w.shape[1:])
        w = half_at(w, 2, c)
        if nx > 2:
            w = jnp.moveaxis(w, 1, 0).reshape(nx, -1, w.shape[-1])
            w = lax.all_to_all(w, "x", 0, 0)
            return jnp.moveaxis(w, 0, 1).reshape(w.shape[1], -1)
        keep, send = half_at(w, 1, x), half_at(w, 1, 1 - x)
        keep, send = (v.reshape(-1, v.shape[-1]) for v in (keep, send))
        got = swap(send, "x")
        return jnp.concatenate([pick(x, (keep, got)), pick(x, (got, keep))], 1)

    wo = collect(across(w_out, head_shape))
    wu = collect(half_at(w_up.reshape(d, 2, -1), 1, c))
    wd = collect(across(w_down, ff_shape))

    seq = y * n + z
    chosen = lax.dynamic_index_in_dim(adapter_index, seq, 0, keepdims=False)

    def select(table):
        return lax.dynamic_index_in_dim(table, chosen, 0, keepdims=False)

    def turned(table):
        return select(jnp.swapaxes(table, 1, 2))

    in_qkv, in_out, in_up, in_down = (turned(t) for t in (ad_in_qkv, ad_in_out, ad_in_up, ad_in_down))
    out_qkv, out_out, out_up, out_down = (select(t) for t in (ad_out_qkv, ad_out_out, ad_out_up, ad_out_down))
    in_out, in_down, out_up = my_heads(in_out, 1), my_ff(in_down, 1), my_ff(out_up, 1)
    out_qkv = my_heads(out_qkv, 2)
    zero = jnp.zeros((r, dl), BF16)
    ao = jnp.concatenate([jnp.concatenate([out_qkv[i] if i == j else zero for j in range(3)], 1) for i in range(3)], 0)
    gains, shifts = norm_gain.astype(F32), norm_bias.astype(F32)
    qvb = my_heads(qv_bias, 1).astype(F32)
    qkv_bias = jnp.concatenate([qvb[0], jnp.zeros((dl,), F32), qvb[1]])[None]
    upb = my_ff(up_bias, 0).astype(F32)[None]
    outb, downb = out_bias.astype(F32)[None], down_bias.astype(F32)[None]

    xs = deal(inputs)
    gs = deal(cotangent)
    rt = 64
    (h1o,) = call(
        norm_kernel,
        (own // rt,),
        [(xs, rows(rt, d)), (gains[0:1], full((1, d))), (shifts[0:1], full((1, d)))],
        [(sds((own, d)), rows(rt, d))],
        "norm1",
    )
    h1 = spread(h1o)
    tile = 256

    np_, _, nq = wq.shape
    qkv, lq = call(
        functools.partial(qkv_kernel, tile),
        (np_,),
        [
            (h1, once((length, d))),
            (wq, pl.BlockSpec((1, d, nq), lambda i: (i, 0, 0))),
            (in_qkv, full((3 * r, d))),
            (ao, cols(3 * r, nq)),
            (qkv_bias, cols(1, nq)),
        ],
        [(sds((length, 3 * dl)), cols(length, nq)), (sds((length, 3 * r)), full((length, 3 * r)))],
        "qkv",
        2 * length * d * 3 * dl,
        2 * d * 3 * dl,
    )
    bq = 256

    def head_cols(base):
        return pl.BlockSpec((length, hd), lambda i: (0, base + i))

    attention_flops = 2 * 2 * heads * length * length * hd
    (ctx,) = call(
        functools.partial(attend_kernel, bq, scale),
        (heads,),
        [(qkv, head_cols(0)), (qkv, head_cols(heads)), (qkv, head_cols(2 * heads))],
        [(sds((length, dl)), head_cols(0))],
        "attend",
        attention_flops,
    )
    nd = wo.shape[2]
    (part_out,) = call(
        functools.partial(down_kernel, tile, d),
        (n,),
        [(ctx, once((length, dl))), (wo, pl.BlockSpec((1, dl, nd), lambda i: (i, 0, 0))), (in_out, full((r, dl)))],
        [(sds((length, wide)), full((length, wide)))],
        "attn_out",
        2 * length * dl * d,
    )
    sum_a, sum_b = gather_sum(part_out)
    mid, h2o, loo = call(
        mid_kernel,
        (own // rt,),
        [
            (xs, rows(rt, d)),
            (sum_a, rows(rt, wide)),
            (sum_b, rows(rt, wide)),
            (outb, full((1, d))),
            (out_out, full((r, d))),
            (gains[1:2], full((1, d))),
            (shifts[1:2], full((1, d))),
        ],
        [(sds((own, d), F32), rows(rt, d)), (sds((own, d)), rows(rt, d)), (sds((own, r)), rows(rt, r))],
        "mid",
    )
    h2 = spread(h2o)
    nu = wu.shape[2]
    act, slope, lu = call(
        functools.partial(up_kernel, tile),
        (n,),
        [
            (h2, once((length, d))),
            (wu, pl.BlockSpec((1, d, nu), lambda i: (i, 0, 0))),
            (in_up, full((r, d))),
            (out_up, cols(r, nu)),
            (upb, cols(1, nu)),
        ],
        [(sds((length, fl)), cols(length, nu)), (sds((length, fl)), cols(length, nu)), (sds((length, r)), full((length, r)))],
        "up",
        2 * length * d * fl,
        2 * d * fl,
    )
    g = spread(gs)
    ft = min(512, fl)
    gpre, gld, t_in_down, t_out_up = call(
        functools.partial(gpre_kernel, tile),
        (fl // ft,),
        [
            (g, once((length, d))),
            (wd, pl.BlockSpec((n, ft, nd), lambda i: (0, i, 0))),
            (slope, cols(length, ft)),
            (act, cols(length, ft)),
            (out_down, full((r, d))),
            (in_down, cols(r, ft)),
            (lu, full((length, r))),
        ],
        [
            (sds((length, fl)), cols(length, ft)),
            (sds((length, r)), full((length, r))),
            (sds((r, fl)), cols(r, ft)),
            (sds((r, fl)), cols(r, ft)),
        ],
        "gpre",
        2 * length * d * fl,
        2 * d * fl,
    )
    dt = 512

    def back(v, w, low, name):
        return call(
            functools.partial(back_kernel, tile, d),
            (d // dt,),
            [
                (v, once(v.shape)),
                (w, pl.BlockSpec((w.shape[0], dt, w.shape[2]), lambda i: (0, i, 0))),
                (low, full(low.shape)),
            ],
            [(sds((length, wide)), full((length, wide)))],
            name,
            2 * length * d * v.shape[1],
            2 * d * v.shape[1],
        )[0]

    gh2_a, gh2_b = gather_sum(back(gpre, wu, out_up, "gh2"))
    (part_down,) = call(
        functools.partial(down_kernel, tile, d),
        (n,),
        [(act, once((length, fl))), (wd, pl.BlockSpec((1, fl, nd), lambda i: (i, 0, 0))), (in_down, full((r, fl)))],
        [(sds((length, wide)), full((length, wide)))],
        "down",
        2 * length * d * fl,
        2 * d * fl,
    )
    gmid, gattno, p_in_up, p_out_out = call(
        gmid_kernel,
        (own // rt,),
        [
            (mid, rows(rt, d)),
            (gs, rows(rt, d)),
            (gh2_a, rows(rt, wide)),
            (gh2_b, rows(rt, wide)),
            (in_up, full((r, d))),
            (gains[1:2], full((1, d))),
            (h2o, rows(rt, d)),
            (loo, rows(rt, r)),
        ],
        [
            (sds((own, d), F32), rows(rt, d)),
            (sds((own, d)), rows(rt, d)),
            (sds((r, d), F32), full((r, d))),
            (sds((r, d), F32), full((r, d))),
        ],
        "gmid",
    )
    gattn = spread(gattno)
    sum_a, sum_b = gather_sum(part_down)
    outs, p_out_down = call(
        out_kernel,
        (own // rt,),
        [
            (mid, rows(rt, d)),
            (sum_a, rows(rt, wide)),
            (sum_b, rows(rt, wide)),
            (downb, full((1, d))),
            (out_down, full((r, d))),
            (gs, rows(rt, d)),
        ],
        [(sds((own, d)), rows(rt, d)), (sds((r, d), F32), full((r, d)))],
        "outputs",
    )
    outputs = undeal(outs)

    gctx, t_in_out, _ = call(
        functools.partial(gctx_kernel, tile),
        (1,),
        [
            (gattn, once((length, d))),
            (wo, once((n, dl, nd))),
            (out_out, full((r, d))),
            (in_out, full((r, dl))),
            (ctx, once((length, dl))),
        ],
        [
            (sds((length, dl)), full((length, dl))),
            (sds((r, dl)), full((r, dl))),
            (sds((length, r)), full((length, r))),
        ],
        "gctx",
        2 * length * d * dl,
    )

    def quarter(v):
        rr = v.shape[0]
        v = v.reshape(rr, nx, 2, dl)
        v = half_at(v, 2, c) + swap(half_at(v, 2, 1 - c), "c")
        if nx > 2:
            return lax.psum_scatter(v, "x", scatter_dimension=1).astype(BF16)
        return (half_at(v, 1, x) + swap(half_at(v, 1, 1 - x), "x")).astype(BF16)

    early = quarter(jnp.concatenate([p_in_up, p_out_out, p_out_down], 0))
    early = jnp.concatenate([t_out_up, t_in_down, t_in_out] + [early[i * r : (i + 1) * r] for i in range(3)], 1)
    everyone = ("y", "z", "x", "c")
    early = lax.all_gather(early, everyone)

    hc = head_cols(0)
    col = pl.BlockSpec((r, hd), lambda i: (0, i))
    gq, gk, gv, tq, tk, tv = call(
        functools.partial(attend_back_kernel, bq, scale),
        (heads,),
        [
            (qkv, head_cols(0)),
            (qkv, head_cols(heads)),
            (qkv, head_cols(2 * heads)),
            (gctx, hc),
            (lq, full((length, 3 * r))),
        ],
        [(sds((length, dl)), hc)] * 3 + [(sds((r, dl)), col)] * 3,
        "attend_back",
        5 * attention_flops // 2,
        scratch=[pltpu.VMEM((length, hd), F32), pltpu.VMEM((length, hd), F32)],
    )
    gqkv = jnp.concatenate([gq, gk, gv], 1)
    sum_a, sum_b = gather_sum(back(gqkv, wq, ao, "gh1"))
    gx, p_in_qkv = call(
        final_kernel,
        (own // rt,),
        [
            (xs, rows(rt, d)),
            (gmid, rows(rt, d)),
            (sum_a, rows(rt, wide)),
            (sum_b, rows(rt, wide)),
            (in_qkv, full((3 * r, d))),
            (gains[0:1], full((1, d))),
            (h1o, rows(rt, d)),
        ],
        [(sds((own, d)), rows(rt, d)), (sds((3 * r, d), F32), full((3 * r, d)))],
        "input_grad",
    )
    input_grad = undeal(gx).astype(F32)
    late = quarter(p_in_qkv)
    late = jnp.concatenate([late, jnp.concatenate([tq, tk, tv], 0)], 1)
    late = lax.all_gather(late, everyone)

    hot = (jnp.arange(na, dtype=jnp.int32)[:, None] == adapter_index[None, :]).astype(BF16)

    def add_up(v):
        v = v.reshape((seqs, nx, 2) + v.shape[1:])
        return jnp.einsum("es,s...->e...", hot, v, preferred_element_type=F32)

    def from_ff(v):
        v = v.reshape(na, nx, 2, r, n, fl // n)
        return v.transpose(0, 3, 4, 1, 2, 5).reshape(na, r, ff)

    def from_heads(v):
        v = v.reshape(na, nx, 2, v.shape[3], heads, hd)
        return v.transpose(0, 3, 4, 1, 2, 5).reshape(na, v.shape[3], d)

    def from_quarters(v):
        return v.transpose(0, 3, 1, 2, 4).reshape(na, v.shape[3], d)

    def turn(v):
        return jnp.swapaxes(v, 1, 2)

    early, late = add_up(early), add_up(late)
    tail = [early[..., 2 * fl + i * dl : 2 * fl + (i + 1) * dl] for i in range(4)]
    g_out_up, g_in_down = from_ff(early[..., :fl]), from_ff(early[..., fl : 2 * fl])
    g_in_out = from_heads(tail[0])
    g_in_up, g_out_out, g_out_down = (from_quarters(v) for v in tail[1:])
    g_in_qkv = from_quarters(late[..., :dl])
    g_out_qkv = from_heads(late[..., dl:]).reshape(na, 3, r, d)
    return (
        outputs,
        input_grad,
        turn(g_in_qkv),
        g_out_qkv,
        turn(g_in_out),
        g_out_out,
        turn(g_in_up),
        g_out_up,
        turn(g_in_down),
        g_out_down,
    )


def solution(mesh):
    act = P(("y", "c"), None, ("z", "x"), None)
    weight = P(None, ("z", "x"))
    ins = (act, P(), P(), weight, P(), weight, P(), weight, P(), weight) + (P(),) * 10 + (act,)

    def program(*arrays):
        ndp, nf = mesh.devices.shape
        ny = ndp // 2
        n = arrays[11].shape[0] // ny
        grid = Mesh(mesh.devices.reshape(ny, 2, n, nf // n), ("y", "c", "z", "x"))
        return jax.shard_map(
            shards,
            mesh=grid,
            in_specs=ins,
            out_specs=(act, act) + (P(),) * 8,
            check_vma=False,
        )(*arrays)

    return program
```

```python
import functools
from types import SimpleNamespace

import jax
import jax.numpy as jnp
from jax import lax
from jax.experimental import pallas as pl
from jax.experimental.pallas import tpu as pltpu
from jax.sharding import Mesh
from jax.sharding import PartitionSpec as P

H = 16
EPS = 1e-05
MASKED = -1e30
F32 = jnp.float32
BF16 = jnp.bfloat16
MESH = pl.DeviceIdType.MESH
ANY = pl.BlockSpec(memory_space=pl.ANY)
WHOLE = pl.BlockSpec(memory_space=pltpu.VMEM)
ROWS = 32
TILE = 256


def nn(a, b):
    return jnp.dot(a, b, preferred_element_type=F32)


def nt(a, b):
    return lax.dot_general(a, b, (((1,), (1,)), ((), ())), preferred_element_type=F32)


def tn(a, b):
    return lax.dot_general(a, b, (((0,), (0,)), ((), ())), preferred_element_type=F32)


def centre(v):
    c = v - jnp.mean(v, -1, keepdims=True)
    rstd = lax.rsqrt(jnp.mean(c * c, -1, keepdims=True) + EPS)
    return c * rstd, rstd


def norm_back(v, grad, gain):
    nh, rstd = centre(v)
    e = gain * grad
    return rstd * (e - jnp.mean(e, -1, keepdims=True) - nh * jnp.mean(nh * e, -1, keepdims=True))


def sds(shape, dtype=BF16):
    return jax.ShapeDtypeStruct(shape, dtype)


def full(shape):
    return pl.BlockSpec(shape, lambda *_: (0,) * len(shape))


def once(shape):
    return pl.BlockSpec(shape, lambda *_: (0,) * len(shape), pipeline_mode=pl.Buffered(1))


def cols(height, tile):
    return pl.BlockSpec((height, tile), lambda i: (0, i))


def run(body, ins, outs, name, grid=(), scratch=None, alias=(), cid=None, flops=0):
    scratch = scratch or {}
    names = list(ins) + list(outs) + list(scratch)

    def kernel(*refs):
        body(SimpleNamespace(**dict(zip(names, refs))))

    params = pltpu.CompilerParams(collective_id=cid, has_side_effects=True) if cid is not None else pltpu.CompilerParams()
    result = pl.pallas_call(
        kernel,
        grid=grid,
        in_specs=[s for _, s in ins.values()],
        out_specs=[s for _, s in outs.values()],
        out_shape=[a for a, _ in outs.values()],
        scratch_shapes=list(scratch.values()),
        input_output_aliases={list(ins).index(a): list(outs).index(b) for a, b in alias},
        compiler_params=params,
        cost_estimate=pl.CostEstimate(flops=flops, bytes_accessed=0, transcendentals=0),
        name=name,
    )(*[a for a, _ in ins.values()])
    return SimpleNamespace(**dict(zip(outs, result)))


def row_loop(count, tile, step):
    @pl.loop(0, count // tile)
    def _(r):
        step(pl.ds(pl.multiple_of(r * tile, tile), tile))


def place():
    return tuple(lax.axis_index(a) for a in ("y", "c", "z", "x"))


def meet(n, axes):
    sem = pltpu.get_barrier_semaphore()
    y, c, z, x = place()
    here = {"y": y, "c": c, "x": x}
    pairs = [a for a in axes if a != "z"]
    for a in pairs:
        pl.semaphore_signal(sem, inc=1, device_id={a: 1 - here[a]}, device_id_type=MESH)
    if "z" in axes:

        @pl.when(z > 0)
        def _():
            pl.semaphore_signal(sem, inc=1, device_id={"z": z - 1}, device_id_type=MESH)

        @pl.when(z < n - 1)
        def _():
            pl.semaphore_signal(sem, inc=1, device_id={"z": z + 1}, device_id_type=MESH)

    count = len(pairs)
    if "z" in axes:
        count += (z + n - 1) // n + (2 * n - 2 - z) // n
    pl.semaphore_wait(sem, count)


def maybe(cond, fn):
    if cond is True:
        fn()
    else:
        pl.when(cond)(fn)


class Sent:
    def __init__(self, links, src, dst, got, where, out_ok=True, in_ok=True):
        k = links.count
        links.count += 1

        def make(src, dst):
            return pltpu.make_async_remote_copy(
                src_ref=src,
                dst_ref=dst,
                send_sem=links.ss.at[k],
                recv_sem=links.rs.at[k],
                device_id=where,
                device_id_type=MESH,
            )

        self.out, self.into = (lambda: make(src(), dst())), (lambda: make(got(), got()))
        self.out_ok, self.in_ok = out_ok, in_ok

    def start(self):
        maybe(self.out_ok, lambda: self.out().start())

    def arrived(self):
        maybe(self.in_ok, lambda: self.into().wait_recv())

    def left(self):
        maybe(self.out_ok, lambda: self.out().wait_send())


class Links:
    def __init__(self, ss, rs):
        self.ss, self.rs, self.count = ss, rs, 0


class Group:
    def __init__(self, copies):
        self.copies = copies

    def start(self):
        for s in self.copies:
            s.start()

    def arrived(self):
        for s in self.copies:
            s.arrived()

    def left(self):
        for s in self.copies:
            s.left()


class Haul:
    def __init__(self, links, w, n, parts=None):
        y, c, z, x = place()
        self.n, self.z = n, z
        self.hops = []
        for t in range(1, n):
            spots = parts if t == 1 and parts else [(None, lambda ref: ref)]
            hop = []
            for src, cut in spots:

                def at(slot, cut=cut):
                    return lambda: cut(w.at[slot, y])

                def source(slot, src=src, cut=cut):
                    return (lambda: src(y)) if src else (lambda: cut(w.at[slot, y]))

                up_ok = jnp.logical_and(z >= t - 1, z < n - 1)
                down_ok = jnp.logical_and(z + t <= n, z >= 1)
                hop.append(Sent(links, source(z - t + 1), at(z - t + 1), at(z - t), {"z": z + 1}, up_ok, z >= t))
                hop.append(Sent(links, source(z + t - 1), at(z + t - 1), at(z + t), {"z": z - 1}, down_ok, z + t <= n - 1))
            self.hops.append(hop)
        self.across = []
        for slot in (z + 1 - 2 * (z % 2), 2 - z // 2, 3 * (1 - z // 2)):

            def mine(slot=slot):
                return w.at[slot, y]

            def other(slot=slot):
                return w.at[slot, 1 - y]

            self.across.append(Sent(links, mine, mine, other, {"y": 1 - y}))
        self.inner = z * (3 - z) == 2
        self.outer = z * (3 - z) == 0

    def hop(self, t):
        return Group(self.hops[t - 1])

    def cross(self, j):
        return self.across[j - 1]

    def when_inner(self, fn):
        pl.when(self.inner)(fn)

    def when_outer(self, fn):
        pl.when(self.outer)(fn)


class Spread:
    def __init__(self, links, mine, out, local):
        y, c, z, x = place()
        me, side, sis, far = c * 2 + x, c * 2 + 1 - x, (1 - c) * 2 + x, (1 - c) * 2 + 1 - x
        self.local = [pltpu.make_async_copy(mine.at[p], out.at[me, p], local.at[p]) for p in range(2)]

        def ref(base, *index):
            return lambda: base.at[index]

        self.xs = [Sent(links, ref(mine, p), ref(out, me, p), ref(out, side, p), {"x": 1 - x}) for p in range(2)]
        self.cs = [Sent(links, ref(mine, p), ref(out, me, p), ref(out, sis, p), {"c": 1 - c}) for p in range(2)]
        self.fs = [Sent(links, ref(out, side, p), ref(out, side, p), ref(out, far, p), {"c": 1 - c}) for p in range(2)]

    def start(self, p):
        self.xs[p].start()
        self.cs[p].start()
        self.local[p].start()

    def relay(self, p):
        self.xs[p].arrived()
        self.fs[p].start()

    def finish(self):
        for p in range(2):
            self.cs[p].arrived()
            self.fs[p].arrived()
            self.local[p].wait()
            for s in (self.xs[p], self.cs[p], self.fs[p]):
                s.left()


class Deal:
    def __init__(self, dsend, drecv, base, src, land, n, zb, per, mb):
        y, c, z, x = place()
        h, zz = z // zb, z % zb
        p = zz % 2
        self.moves = []
        for m in range(mb):
            tc, tz = zz // 2, (c * mb + m) * per + h
            away = jnp.logical_or(tc != c, tz != z)
            far = pltpu.make_async_remote_copy(
                src_ref=src.at[0, m],
                dst_ref=land.at[p],
                send_sem=dsend.at[base + m],
                recv_sem=drecv.at[base + p],
                device_id={"c": tc, "z": tz},
                device_id_type=MESH,
            )
            near = pltpu.make_async_copy(src.at[0, m], land.at[p], drecv.at[base + p])
            self.moves.append((away, far, near))
        self.gets = []
        for q in range(2):
            sz = (z % per) * zb + 2 * c + q
            away = jnp.logical_or(z // (per * mb) != c, sz != z)
            m = (z // per) % mb
            far = pltpu.make_async_remote_copy(
                src_ref=land.at[q],
                dst_ref=land.at[q],
                send_sem=dsend.at[base + q],
                recv_sem=drecv.at[base + q],
                device_id={"c": z // (per * mb), "z": sz},
                device_id_type=MESH,
            )
            near = pltpu.make_async_copy(src.at[0, m], land.at[q], drecv.at[base + q])
            self.gets.append((away, far, near))

    def start(self):
        for away, far, near in self.moves:
            pl.when(away)(lambda far=far: far.start())
            pl.when(jnp.logical_not(away))(lambda near=near: near.start())

    def arrived(self):
        for away, far, near in self.gets:
            pl.when(away)(lambda far=far: far.wait_recv())
            pl.when(jnp.logical_not(away))(lambda near=near: near.wait())

    def left(self):
        for away, far, near in self.moves:
            pl.when(away)(lambda far=far: far.wait_send())


class Undeal:
    def __init__(self, dsend, drecv, base, mine, out, n, zb, per, mb):
        y, c, z, x = place()
        m = (z // per) % mb
        self.moves = []
        for p in range(2):
            tc, tz = z // (per * mb), (z % per) * zb + 2 * c + p
            away = jnp.logical_or(tc != c, tz != z)
            far = pltpu.make_async_remote_copy(
                src_ref=mine.at[p],
                dst_ref=out.at[0, m],
                send_sem=dsend.at[base + p],
                recv_sem=drecv.at[base + m],
                device_id={"c": tc, "z": tz},
                device_id_type=MESH,
            )
            near = pltpu.make_async_copy(mine.at[p], out.at[0, m], drecv.at[base + m])
            self.moves.append((away, far, near))
        self.gets = []
        h, zz = z // zb, z % zb
        for q in range(mb):
            sc, sz = zz // 2, (c * mb + q) * per + h
            away = jnp.logical_or(sc != c, sz != z)
            far = pltpu.make_async_remote_copy(
                src_ref=out.at[0, q],
                dst_ref=out.at[0, q],
                send_sem=dsend.at[base + q],
                recv_sem=drecv.at[base + q],
                device_id={"c": sc, "z": sz},
                device_id_type=MESH,
            )
            near = pltpu.make_async_copy(mine.at[zz % 2], out.at[0, q], drecv.at[base + q])
            self.gets.append((away, far, near))

    start = Deal.start
    arrived = Deal.arrived
    left = Deal.left


def crowd(n, axes=()):
    sem = pltpu.get_barrier_semaphore()
    y, c, z, x = place()
    here = {"y": y, "x": x}
    for cc in range(2):
        for zz in range(n):

            @pl.when(jnp.logical_or(c != cc, z != zz))
            def _(cc=cc, zz=zz):
                pl.semaphore_signal(sem, inc=1, device_id={"c": cc, "z": zz}, device_id_type=MESH)

    for a in axes:
        pl.semaphore_signal(sem, inc=1, device_id={a: 1 - here[a]}, device_id_type=MESH)
    pl.semaphore_wait(sem, 2 * n - 1 + len(axes))


def links_scratch(count):
    return {"ss": pltpu.SemaphoreType.DMA((count,)), "rs": pltpu.SemaphoreType.DMA((count,))}


def gather_body(n, zb, per, mb, r):
    y, c, z, x = place()
    hd = r.qs.shape[2] // 2
    uc, dc = r.us.shape[2], r.ds.shape[3]
    half = r.qs.shape[1]
    crowd(n, ("x", "y"))
    links = Links(r.ss, r.rs)
    deal_x = Deal(r.dsend, r.drecv, 0, r.inputs, r.xv, n, zb, per, mb)
    deal_g = Deal(r.dsend, r.drecv, 2, r.cot, r.gv, n, zb, per, mb)
    deal_x.start()

    def lanes(start, size):
        return pl.ds(pl.multiple_of(start, 128), size)

    stage = [
        pltpu.make_async_copy(r.wq_in.at[:, :, lanes(c * hd, hd)], r.qs.at[:, :, 0:hd], r.ls.at[0]),
        pltpu.make_async_copy(r.wq_in.at[:, :, lanes((c + 4) * hd, hd)], r.qs.at[:, :, hd : 2 * hd], r.ls.at[1]),
        pltpu.make_async_copy(r.wo_in.at[:, :, x, c], r.os, r.ls.at[2]),
        pltpu.make_async_copy(r.wu_in.at[:, :, lanes(c * uc, uc)], r.us, r.ls.at[3]),
        pltpu.make_async_copy(r.wd_in.at[:, :, x, c], r.ds, r.ls.at[4]),
    ]
    for s in stage:
        s.start()

    def q_keep(ref):
        return ref.at[..., lanes(hd * x, 2 * hd)]

    def q_got(ref):
        return ref.at[..., lanes(2 * hd * (1 - x), hd)]

    def q_give(ref):
        return ref.at[..., lanes(2 * hd * x, hd)]

    def d_keep(ref):
        return ref.at[..., lanes(dc * x, dc)]

    def d_got(ref):
        return ref.at[..., lanes(dc * (1 - x), dc)]

    side = {"x": 1 - x}
    swap_q = Sent(
        links, lambda: r.wq_in.at[:, :, lanes((c + 2) * hd, hd)], lambda: q_give(r.wq.at[z]), lambda: q_got(r.wq.at[z]), side
    )
    swap_o = Sent(links, lambda: r.wo_in.at[:, :, 1 - x, c], lambda: d_keep(r.wo.at[z]), lambda: d_got(r.wo.at[z]), side)
    swap_d = Sent(links, lambda: r.wd_in.at[:, :, 1 - x, c], lambda: d_keep(r.wd.at[z]), lambda: d_got(r.wd.at[z]), side)
    swap_q.start()
    swap_o.start()
    haul_q = Haul(links, r.wq, n, [(lambda y: r.qs.at[y], q_keep), (None, q_got)])
    haul_o = Haul(links, r.wo, n, [(lambda y: r.os.at[y], d_keep), (None, d_got)])
    spread = Spread(links, r.hv, r.h1, r.lh)
    for s in stage:
        s.wait()
    q1, o1 = haul_q.hop(1).copies, haul_o.hop(1).copies
    Group(q1[:2]).start()
    Group(o1[:2]).start()
    keep = [
        pltpu.make_async_copy(r.qs, q_keep(r.wq.at[z]), r.ls.at[0]),
        pltpu.make_async_copy(r.os, d_keep(r.wo.at[z]), r.ls.at[1]),
        pltpu.make_async_copy(r.us, r.wu.at[z], r.ls.at[2]),
        pltpu.make_async_copy(r.ds, d_keep(r.wd.at[z]), r.ls.at[3]),
    ]
    for s in keep:
        s.start()
    swap_q.arrived()
    Group(q1[2:]).start()
    swap_o.arrived()
    Group(o1[2:]).start()

    deal_x.arrived()
    tok = r.xv.shape[1]
    for p in range(2):

        @pl.loop(0, tok // ROWS)
        def _(i):
            at = pl.ds(pl.multiple_of(i * ROWS, ROWS), ROWS)
            v = r.xv[p, at, :]
            r.xs[p, at, :] = v
            nh, _ = centre(v.astype(F32))
            h = (nh * r.gain[...] + r.shift[...]).astype(BF16)
            r.hv[p, at, :] = h

        spread.start(p)
    swap_d.start()

    def step(haul, t):
        haul.hop(t).arrived()
        if t < n - 1:
            haul.hop(t + 1).start()
        if t == 1:
            haul.cross(1).start()
            haul.when_inner(haul.cross(2).start)
        if t == 2:
            haul.when_outer(haul.cross(2).start)
            haul.when_inner(haul.cross(3).start)
        if t == 3:
            haul.when_outer(haul.cross(3).start)

    step(haul_q, 1)
    step(haul_o, 1)
    spread.relay(0)
    spread.relay(1)
    step(haul_q, 2)
    step(haul_o, 2)
    deal_g.start()
    step(haul_q, 3)
    step(haul_o, 3)
    spread.finish()
    deal_g.arrived()
    for p in range(2):
        r.gs[p] = r.gv[p]
    swap_d.arrived()
    for s in keep:
        s.wait()
    for haul in (haul_q, haul_o):
        for j in (1, 2, 3):
            haul.cross(j).arrived()
            haul.cross(j).left()
        for t in (1, 2, 3):
            haul.hop(t).left()
    for s in (swap_q, swap_o, swap_d):
        s.left()
    deal_x.left()
    deal_g.left()


def edges(first, last):
    count = pl.num_programs(0)
    if first:
        pl.when(pl.program_id(0) == 0)(first)
    return lambda: pl.when(pl.program_id(0) == count - 1)(last) if last else None


def qkv_body(r, first=None, last=None):
    close = edges(first, last)
    new = pl.program_id(0) == 0

    def step(at):
        @pl.when(new)
        def _():
            r.lq[at, :] = nt(r.h[at, :], r.low_in[...]).astype(BF16)

        acc = nn(r.h[at, :], r.w[0]) + nn(r.lq[at, :], r.low_out[...])
        r.out[at, :] = (acc + r.bias[...]).astype(BF16)

    row_loop(r.h.shape[0], TILE, step)
    close()


def up_body(r, first=None, last=None):
    close = edges(first, last)
    new = pl.program_id(0) == 0

    def step(at):
        @pl.when(new)
        def _():
            r.lu[at, :] = nt(r.h[at, :], r.low_in[...]).astype(BF16)

        pre = nn(r.h[at, :], r.w[0]) + nn(r.lu[at, :], r.low_out[...]) + r.bias[...]
        cdf = 0.5 * (1.0 + lax.erf(pre * (0.5**0.5)))
        pdf = jnp.exp(-0.5 * pre * pre) * 0.3989422804014327
        r.act[at, :] = (pre * cdf).astype(BF16)
        r.slope[at, :] = (cdf + pre * pdf).astype(BF16)

    row_loop(r.h.shape[0], TILE, step)
    close()


def gpre_body(r):
    new = pl.program_id(0) == 0
    parts, nc = r.w.shape[0], r.w.shape[2]

    def step(at):
        @pl.when(new)
        def _():
            r.gld[at, :] = nt(r.g[at, :], r.low_out[...]).astype(BF16)

        acc = nn(r.gld[at, :], r.low_in[...])
        for p in range(parts):
            acc += nt(r.g[at, p * nc : (p + 1) * nc], r.w[p])
        r.gpre[at, :] = (acc * r.slope[at, :].astype(F32)).astype(BF16)

    row_loop(r.g.shape[0], TILE, step)
    r.tin[...] = tn(r.gld[...], r.act[...]).astype(BF16)
    r.tout[...] = tn(r.lu[...], r.gpre[...]).astype(BF16)


def gctx_body(quarter, r):
    parts, nc = r.w.shape[0], r.w.shape[2]
    dl = r.ctx.shape[1]

    def step(at):
        glo = nt(r.g[at, :], r.low_out[...]).astype(BF16)
        r.glo[at, :] = glo
        acc = nn(glo, r.low_in[...])
        for p in range(parts):
            acc += nt(r.g[at, p * nc : (p + 1) * nc], r.w[p])
        r.gctx[at, :] = acc.astype(BF16)

    row_loop(r.g.shape[0], TILE, step)
    r.tin[...] = tn(r.glo[...], r.ctx[...]).astype(BF16)
    mine = pl.ds(pl.multiple_of(quarter() * dl, dl), dl)
    r.tout[...] = tn(r.lo[...], r.g[:, mine]).astype(BF16)


def forward_block(src, w, out, at):
    nc = w.shape[2]

    @pl.loop(0, w.shape[0])
    def _(i):
        out[:, pl.ds(pl.multiple_of(i * nc, nc), nc)] = nn(src[at, :], w[i]).astype(BF16)


def backward_block(src, w, out, at):
    parts, d, nc = w.shape
    dt = min(512, d)

    @pl.loop(0, d // dt)
    def _(i):
        rows = pl.ds(pl.multiple_of(i * dt, dt), dt)
        acc = nt(src[at, 0:nc], w[0, rows, :])
        for p in range(1, parts):
            acc += nt(src[at, p * nc : (p + 1) * nc], w[p, rows, :])
        out[:, rows] = acc.astype(BF16)


def plain_product_body(block, r):
    own = TILE

    @pl.loop(0, r.a.shape[0] // own)
    def _(t):
        at = pl.ds(pl.multiple_of(t * own, own), own)
        block(r.a, r.w, r.out.at[at, :], at)


def product_body(block, extra, axes, n, own_rows, after, begin, end, r):
    y, c, z, x = place()
    own = r.part.shape[1]
    rank = r.low.shape[0]
    tok = own // 2
    if "plane" in axes:
        crowd(n, ("x",))
    else:
        meet(n, axes)
    links = Links(r.ss, r.rs)
    ctx = begin(r, links) if begin else None

    def ref(base, *index):
        return lambda: base.at[index] if index else base

    send_low1 = Sent(links, ref(r.low1, 0), ref(r.low1, 1), ref(r.low1, 1), {"c": 1 - c})
    send_low2 = Sent(links, ref(r.low2, 0), ref(r.low2, 1), ref(r.low2, 1), {"x": 1 - x})
    send_a = Sent(links, ref(r.part, 0), ref(r.got, 0), ref(r.got, 0), {"c": 1 - c})
    send_c = Sent(links, ref(r.part, 2), ref(r.got, 1), ref(r.got, 1), {"c": 1 - c})

    def half(base, index, p):
        return lambda: base.at[index, pl.ds(p * tok, tok)]

    send_b = [Sent(links, half(r.got, 2, p), half(r.got, 3, p), half(r.got, 3, p), {"x": 1 - x}) for p in range(2)]

    low_cols = r.low1.shape[2]

    def low_step(at):
        v = nt(r.a[at, :], r.low[...])
        pad = jnp.zeros((v.shape[0], low_cols - rank), F32)
        r.low1[0, at, :] = jnp.concatenate([v, pad], 1).astype(BF16)

    row_loop(r.a.shape[0], TILE, low_step)
    send_low1.start()

    @pl.loop(0, 4)
    def _(t):
        cc = jnp.where(t % 2 == 0, 1 - c, c)
        xx = jnp.where(t < 2, 1 - x, x)
        at = pl.ds(pl.multiple_of((cc * 2 + xx) * own, own), own)
        block(r.a, r.w, r.part.at[t], at)

        @pl.when(t == 0)
        def _():
            send_a.start()
            send_low1.arrived()
            r.low2[0] = (r.low1[0].astype(F32) + r.low1[1].astype(F32)).astype(BF16)
            send_low2.start()

        @pl.when(t == 1)
        def _():
            send_a.arrived()
            for p in range(2):

                @pl.loop(0, tok // ROWS)
                def _(i):
                    at = pl.ds(pl.multiple_of(p * tok + i * ROWS, ROWS), ROWS)
                    r.got[2, at, :] = (r.part[1, at, :].astype(F32) + r.got[0, at, :].astype(F32)).astype(BF16)

                send_b[p].start()

        @pl.when(t == 2)
        def _():
            send_c.start()

    send_low2.arrived()
    r.lows[...] = (r.low2[0].astype(F32) + r.low2[1].astype(F32)).astype(BF16)[:, :rank]
    if extra:
        extra(r, (x * 2 + c))
    send_c.arrived()
    for p in range(2):
        send_b[p].arrived()

        @pl.loop(0, tok // ROWS)
        def _(i):
            at = pl.ds(pl.multiple_of(p * tok + i * ROWS, ROWS), ROWS)
            s = r.part[3, at, :].astype(F32) + r.got[1, at, :].astype(F32) + r.got[3, at, :].astype(F32)
            low_at = pl.ds(pl.multiple_of((c * 2 + x) * own + p * tok + i * ROWS, ROWS), ROWS)
            own_rows(r, p, pl.ds(pl.multiple_of(i * ROWS, ROWS), ROWS), s, r.lows[low_at, :])

        if after:
            after(r, ctx, p)
    if end:
        end(r, ctx)
    for s in [send_low1, send_low2, send_a, send_c] + send_b:
        s.left()


def mid_rows(r, p, at, s, low):
    mid = r.x[p, at, :].astype(F32) + s + r.bias[...] + nn(low, r.low_out[...])
    r.mid[p, at, :] = mid
    nh, _ = centre(mid)
    r.hv[p, at, :] = (nh * r.gain[...] + r.shift[...]).astype(BF16)


def out_rows(r, p, at, s, low):
    r.ov[p, at, :] = (r.mid[p, at, :] + s + r.bias[...] + nn(low, r.low_out[...])).astype(BF16)


def gmid_rows(r, p, at, s, low):
    gh = s + nn(low, r.low_in[...])
    gmid = r.g[p, at, :].astype(F32) + norm_back(r.mid[p, at, :], gh, r.gain[...])
    r.gmid[p, at, :] = gmid
    r.hv[p, at, :] = gmid.astype(BF16)


def final_rows(r, p, at, s, low):
    gh = s + nn(low, r.low_in[...])
    r.ov[p, at, :] = (r.gmid[p, at, :] + norm_back(r.x[p, at, :].astype(F32), gh, r.gain[...])).astype(BF16)


def low_term(r, dev):
    dl = r.term.shape[1]
    r.term[...] = tn(r.lows[...], r.full[...]).astype(BF16)


def places(length, tok, nx):
    spots = []
    for b in range(length // tok):
        lead, xx = divmod(b, nx)
        cc, p = divmod(lead, 2)
        spots.append(((cc * nx + xx) * 2 + p) * tok)
    return spots


def in_order(ref, out, spots, tok):
    for b, at in enumerate(spots):
        out[b * tok : (b + 1) * tok, :] = ref[at : at + tok, :]


def softmax_block(q, k, start, scale):
    s = nt(q, k) * scale
    r = lax.broadcasted_iota(jnp.int32, s.shape, 0) + start
    c = lax.broadcasted_iota(jnp.int32, s.shape, 1)
    s = jnp.where(r >= c, s, MASKED)
    p = jnp.exp(s - jnp.max(s, -1, keepdims=True))
    return p * (1.0 / jnp.sum(p, -1, keepdims=True))


def attend_body(bq, tok, spots, scale, r, first=None, last=None):
    close = edges(first, last)
    length = r.q.shape[0]
    for ref, out in ((r.q, r.qn), (r.k, r.kn), (r.v, r.vn)):
        in_order(ref, out, spots, tok)
    for start in range(0, length, bq):
        end = start + bq
        p = softmax_block(r.qn[start:end, :], r.kn[:end, :], start, scale)
        ctx = nn(p.astype(BF16), r.vn[:end, :]).astype(BF16)
        for i in range(bq // tok):
            at = spots[start // tok + i]
            r.ctx[at : at + tok, :] = ctx[i * tok : (i + 1) * tok]
    close()


def attend_back_body(bq, tok, spots, scale, r):
    length, hd = r.q.shape
    heads = pl.num_programs(0)
    rank = r.terms.shape[1]
    head = pl.program_id(0)
    gq, gk, gv = (r.out.at[:, pl.ds(pl.multiple_of((i * heads + head) * hd, hd), hd)] for i in range(3))
    for ref, out in ((r.q, r.qn), (r.k, r.kn), (r.v, r.vn), (r.g, r.gn)):
        in_order(ref, out, spots, tok)
    for start in reversed(range(0, length, bq)):
        end = start + bq
        q, g = r.qn[start:end, :], r.gn[start:end, :]
        p = softmax_block(q, r.kn[:end, :], start, scale)
        dp = nt(g, r.vn[:end, :])
        ds = (p * (dp - jnp.sum(p * dp, -1, keepdims=True))).astype(BF16)
        gq_here = (nn(ds, r.kn[:end, :]) * scale).astype(BF16)
        for i in range(bq // tok):
            at = spots[start // tok + i]
            gq[at : at + tok, :] = gq_here[i * tok : (i + 1) * tok]
        dk, dv = tn(ds, q), tn(p.astype(BF16), g)
        if end == length:
            r.ks[...] = dk
            r.vs[...] = dv
        else:
            r.ks[:end, :] += dk
            r.vs[:end, :] += dv
    for b, at in enumerate(spots):
        here = slice(b * tok, (b + 1) * tok)
        gk[at : at + tok, :] = (r.ks[here, :] * scale).astype(BF16)
        gv[at : at + tok, :] = r.vs[here, :].astype(BF16)
    for i, ref in enumerate((gq, gk, gv)):
        r.terms[i] = tn(r.lq[:, i * rank : (i + 1) * rank], ref[...]).astype(BF16)


def add_up_body(unit, r):
    e = pl.program_id(0)
    seqs, devs = r.early.shape[0], r.early.shape[1]
    d, ff = r.ino.shape[2], r.outu.shape[2]
    dl, fl, hd = d // devs, ff // devs, d // H
    for ref in (r.inq, r.outq, r.ino, r.outo, r.inu, r.outu, r.ind, r.outd):
        ref[...] = jnp.zeros_like(ref)

    @pl.loop(0, seqs)
    def _(q):
        @pl.when(r.index[q] == e)
        def _():
            for dev in range(devs):

                def add(ref, at, width, source, start, dev=dev):
                    ref[0, :, at : at + width] += source[q, dev, :, start : start + width].astype(F32)

                for i in range(fl // unit):
                    add(r.outu, (i * devs + dev) * unit, unit, r.early, i * unit)
                    add(r.ind, (i * devs + dev) * unit, unit, r.early, fl + i * unit)
                for i in range(dl // hd):
                    add(r.ino, (i * devs + dev) * hd, hd, r.early, 2 * fl + i * hd)
                    add(r.outq, (i * devs + dev) * hd, hd, r.middle, i * hd)
                for i, ref in enumerate((r.inu, r.outo, r.outd)):
                    add(ref, dev * dl, dl, r.early, 2 * fl + (1 + i) * dl)
                add(r.inq, dev * dl, dl, r.late, 0)


def shards(
    inputs,
    norm_gain,
    norm_bias,
    w_qkv,
    qv_bias,
    w_out,
    out_bias,
    w_up,
    up_bias,
    w_down,
    down_bias,
    adapter_index,
    ad_in_qkv,
    ad_out_qkv,
    ad_in_out,
    ad_out_out,
    ad_in_up,
    ad_out_up,
    ad_in_down,
    ad_out_down,
    cotangent,
):
    y, c, z, x = (lax.axis_index(a) for a in ("y", "c", "z", "x"))
    ny, n, nx = lax.axis_size("y"), lax.axis_size("z"), lax.axis_size("x")
    group = 2 * nx
    mb, tok, d = inputs.shape[1:]
    rank = ad_out_out.shape[1]
    na = ad_in_qkv.shape[0]
    hd = d // H
    heads = H // group
    dl = d // group
    ff = up_bias.shape[0]
    fl = ff // group
    unit = fl // n
    seqs = adapter_index.shape[0]
    length = 2 * ny * mb * n * nx * tok // seqs
    zb = length // tok // nx
    per = n // zb
    own = length // group
    scale = hd**-0.5
    dev = x * 2 + c
    fast = nx == 2 and n == 4 and ny == 2
    assert zb == 4 and n == 2 * mb * per and mb == 2 and own == 2 * tok
    everyone = ("y", "z", "x", "c")
    plan = (n, zb, per, mb)

    def half_at(v, axis, index):
        return lax.dynamic_index_in_dim(v, index, axis, keepdims=False)

    def part(v, shape, lead):
        v = v.reshape(v.shape[:lead] + shape + v.shape[lead + 1 :])
        v = half_at(v, lead + 1, x)
        return half_at(v, lead + 1, c)

    ff_shape, head_shape = (n, nx, 2, unit), (heads, nx, 2, hd)

    def my_ff(v, axis):
        w = part(v, ff_shape, axis)
        return w.reshape(w.shape[:axis] + (fl,) + w.shape[axis + 2 :])

    def my_heads(v, axis):
        w = part(v, head_shape, axis)
        return w.reshape(w.shape[:axis] + (dl,) + w.shape[axis + 2 :])

    seq = y * n + z
    chosen = lax.dynamic_index_in_dim(adapter_index, seq, 0, keepdims=False)

    def select(table):
        return lax.dynamic_index_in_dim(table, chosen, 0, keepdims=False)

    def turned(table):
        return select(jnp.swapaxes(table, 1, 2))

    in_qkv, in_out, in_up, in_down = (turned(t) for t in (ad_in_qkv, ad_in_out, ad_in_up, ad_in_down))
    out_qkv, out_out, out_up, out_down = (select(t) for t in (ad_out_qkv, ad_out_out, ad_out_up, ad_out_down))
    in_out, in_down, out_up = my_heads(in_out, 1), my_ff(in_down, 1), my_ff(out_up, 1)
    out_qkv = my_heads(out_qkv, 2)
    zero = jnp.zeros((rank, dl), BF16)
    ao = jnp.concatenate([jnp.concatenate([out_qkv[i] if i == j else zero for j in range(3)], 1) for i in range(3)], 0)
    gains, shifts = norm_gain.astype(F32), norm_bias.astype(F32)
    qvb = my_heads(qv_bias, 1).astype(F32)
    qkv_bias = jnp.concatenate([qvb[0], jnp.zeros((dl,), F32), qvb[1]])[None]
    upb = my_ff(up_bias, 0).astype(F32)[None]
    outb, downb = out_bias.astype(F32)[None], down_bias.astype(F32)[None]

    row2 = (2, tok, d)
    blocks = (group, 2, tok, d)
    vec = full((1, d))

    def slow_deal(v):
        v = lax.all_gather(v[0], ("c", "z"))
        cs, h, m = z // (per * mb), z % per, (z // per) % mb
        return jnp.stack([half_at(half_at(v, 0, cs * n + h * zb + 2 * c + p), 0, m) for p in range(2)])

    def slow_undeal(v):
        v = lax.all_gather(v.reshape(row2), ("c", "z"))
        h, zz = z // zb, z % zb
        at = [(zz // 2) * n + (c * mb + m) * per + h for m in range(mb)]
        return jnp.stack([half_at(half_at(v, 0, a), 0, zz % 2) for a in at])[None]

    def slow_spread(v):
        return lax.all_gather(v.reshape(own, d), ("c", "x"), tiled=True)

    def slow_sum(v):
        return lax.psum_scatter(v.astype(F32), ("c", "x"), scatter_dimension=0, tiled=True)

    if fast:
        cut = (2, d // 2)
        k0 = run(
            functools.partial(gather_body, *plan),
            dict(
                inputs=(inputs, ANY),
                cot=(cotangent, ANY),
                wq_in=(w_qkv.reshape(2, d // 2, -1), ANY),
                wo_in=(w_out.reshape(2, heads // 2, 2, 2, hd, -1), ANY),
                wu_in=(w_up.reshape(2, d // 2, -1), ANY),
                wd_in=(w_down.reshape(2, n // 2, 2, 2, unit, -1), ANY),
                gain=(gains[0:1], WHOLE),
                shift=(shifts[0:1], WHOLE),
            ),
            dict(
                wq=(sds((n, 2, d // 2, 3 * hd)), ANY),
                wo=(sds((n, 2, heads // 2, hd, d // n)), ANY),
                wu=(sds((n, 2, d // 2, unit)), ANY),
                wd=(sds((n, 2, n // 2, unit, d // n)), ANY),
                h1=(sds(blocks), ANY),
                xs=(sds(row2), WHOLE),
                gs=(sds(row2), WHOLE),
            ),
            "gather",
            scratch=dict(
                xv=pltpu.VMEM(row2, BF16),
                gv=pltpu.VMEM(row2, BF16),
                hv=pltpu.VMEM(row2, BF16),
                qs=pltpu.VMEM((2, d // 2, 2 * hd), BF16),
                os=pltpu.VMEM((2, heads // 2, hd, d // (2 * n)), BF16),
                us=pltpu.VMEM((2, d // 2, unit), BF16),
                ds=pltpu.VMEM((2, n // 2, unit, d // (2 * n)), BF16),
                ls=pltpu.SemaphoreType.DMA((5,)),
                lh=pltpu.SemaphoreType.DMA((2,)),
                dsend=pltpu.SemaphoreType.DMA((4,)),
                drecv=pltpu.SemaphoreType.DMA((4,)),
                **links_scratch(40),
            ),
            cid=0,
        )
        xs, gs = k0.xs, k0.gs
        wq, wo = k0.wq.reshape(n, d, 3 * hd), k0.wo.reshape(n, dl, d // n)
        wu, wd = k0.wu, k0.wd
        h1 = k0.h1.reshape(length, d)
    else:
        xs, gs = slow_deal(inputs), slow_deal(cotangent)
        nh, _ = centre(xs.astype(F32))
        h1 = slow_spread((nh * gains[0] + shifts[0]).astype(BF16))
        wq = lax.all_gather(w_qkv, ("z", "x"), axis=1, tiled=True)
        wq = part(wq.reshape(d, 3, d), head_shape, 2).reshape(1, d, 3 * dl)

        def across(w, shape):
            w = half_at(w.reshape(shape + w.shape[1:]), 2, c)
            w = jnp.moveaxis(w, 1, 0).reshape(nx, -1, w.shape[-1])
            w = lax.all_to_all(w, "x", 0, 0)
            w = jnp.moveaxis(w, 0, 1).reshape(w.shape[1], -1)
            return lax.all_gather(w, "z")

        wo, wd = across(w_out, head_shape), across(w_down, ff_shape)
        wu = lax.all_gather(half_at(w_up.reshape(d, 2, -1), 1, c), "z")

    def carried(**arrays):
        ins = {k + "_in": (v, ANY) for k, v in arrays.items()}
        outs = {k: (sds(v.shape), ANY) for k, v in arrays.items()}
        return ins, outs, [(k + "_in", k) for k in arrays]

    np_, _, nq = wq.shape
    qkv_ins = dict(
        h=(h1, once((length, d))),
        w=(wq, pl.BlockSpec((1, d, nq), lambda i: (i, 0, 0))),
        low_in=(in_qkv, full((3 * rank, d))),
        low_out=(ao, cols(3 * rank, nq)),
        bias=(qkv_bias, cols(1, nq)),
    )
    qkv_outs = dict(out=(sds((length, 3 * dl)), cols(length, nq)), lq=(sds((length, 3 * rank)), full((length, 3 * rank))))
    if fast:
        ins, outs, alias = carried(wu=wu)

        def qkv_carry(r):
            hop = Haul(Links(r.ss, r.rs), r.wu, n).hop(1)

            def first():
                meet(n, ("z",))
                hop.start()

            def last():
                hop.arrived()
                hop.left()

            qkv_body(r, first, last)

        k1 = run(
            qkv_carry, {**qkv_ins, **ins}, {**qkv_outs, **outs}, "qkv", (np_,), links_scratch(9), alias, 1, 2 * length * d * 3 * dl
        )
        wu = k1.wu
    else:
        k1 = run(qkv_body, qkv_ins, qkv_outs, "qkv", (np_,))
    qkv, lq = k1.out, k1.lq

    bq = 256
    spots = places(length, tok, nx)
    setup = (bq, tok, spots, scale)

    def head_cols(base):
        return pl.BlockSpec((length, hd), lambda i: (0, base + i))

    def head_scratch(names):
        return {k: pltpu.VMEM((length, hd), BF16) for k in names}

    att_ins = dict(q=(qkv, head_cols(0)), k=(qkv, head_cols(heads)), v=(qkv, head_cols(2 * heads)))
    att_outs = dict(ctx=(sds((length, dl)), head_cols(0)))
    att_flops = 2 * heads * length * length * hd
    if fast:
        ins, outs, alias = carried(wu=wu)
        ins["gs"], outs["g"] = (gs, once(row2)), (sds(blocks), ANY)

        def attend_carry(r):
            links = Links(r.ss, r.rs)
            haul = Haul(links, r.wu, n)
            spread = Spread(links, r.gs, r.g, r.lh)

            def first():
                meet(n, ("z", "y", "x", "c"))
                haul.hop(2).start()
                haul.cross(1).start()
                haul.when_inner(haul.cross(2).start)
                spread.start(0)
                spread.start(1)

            def last():
                spread.relay(0)
                spread.relay(1)
                haul.hop(2).arrived()
                haul.hop(2).left()
                haul.cross(1).arrived()
                haul.cross(1).left()
                haul.when_inner(haul.cross(2).arrived)
                haul.when_inner(haul.cross(2).left)
                spread.finish()

            attend_body(*setup, r, first, last)

        k2 = run(
            attend_carry,
            {**att_ins, **ins},
            {**att_outs, **outs},
            "attend",
            (heads,),
            {**head_scratch(("qn", "kn", "vn")), "lh": pltpu.SemaphoreType.DMA((2,)), **links_scratch(15)},
            alias,
            2,
            att_flops,
        )
        wu, g = k2.wu, k2.g.reshape(length, d)
    else:
        k2 = run(functools.partial(attend_body, *setup), att_ins, att_outs, "attend", (heads,), head_scratch(("qn", "kn", "vn")))
        g = slow_spread(gs)
    ctx = k2.ctx

    def low_ins(a, w, low):
        return dict(a=(a, WHOLE), w=(w, WHOLE), low=(low, WHOLE))

    def sum_scratch(more):
        return dict(
            part=pltpu.VMEM((4, own, d), BF16),
            got=pltpu.VMEM((4, own, d), BF16),
            low1=pltpu.VMEM((2, length, 128), BF16),
            low2=pltpu.VMEM((2, length, 128), BF16),
            lh=pltpu.SemaphoreType.DMA((2,)),
            **more,
        )

    def group_low(a, low):
        return lax.psum(jnp.dot(a, low.T, preferred_element_type=F32), ("c", "x")).astype(BF16)

    def slow_product(block, a, w, name):
        out = run(
            functools.partial(plain_product_body, block),
            dict(a=(a, WHOLE), w=(w, WHOLE)),
            dict(out=(sds((length, d)), WHOLE)),
            name,
        ).out
        return slow_sum(out)

    def mine(v):
        return lax.dynamic_slice_in_dim(v, (c * nx + x) * own, own, 0)

    def quarter(v):
        return lax.dynamic_slice_in_dim(v, dev * dl, dl, 1)

    def slow_term(low, v):
        return lax.dot_general(low, v, (((0,), (0,)), ((), ())), preferred_element_type=F32).astype(BF16)

    def dot(a, b):
        return jnp.dot(a, b, preferred_element_type=F32)

    if fast:
        ins, outs, alias = carried(wu=wu, wd=wd)

        def begin(r, links):
            hu, hdn = Haul(links, r.wu, n), Haul(links, r.wd, n, [(None, lambda ref: ref)])
            hu.hop(3).start()
            hu.when_outer(hu.cross(2).start)
            hu.when_inner(hu.cross(3).start)
            hdn.hop(1).start()
            return SimpleNamespace(hu=hu, hd=hdn, spread=Spread(links, r.hv, r.h, r.lh))

        def after(r, k, p):
            k.spread.start(p)
            if p == 0:
                k.hu.hop(3).arrived()
                k.hu.when_outer(k.hu.cross(3).start)
                k.hd.hop(1).arrived()
                k.hd.hop(2).start()
                k.hd.cross(1).start()
                k.hd.when_inner(k.hd.cross(2).start)

        def end(r, k):
            k.spread.relay(0)
            k.spread.relay(1)
            k.spread.finish()
            k.hu.hop(3).left()
            k.hu.when_outer(k.hu.cross(2).arrived)
            k.hu.when_outer(k.hu.cross(2).left)
            k.hu.cross(3).arrived()
            k.hu.cross(3).left()
            k.hd.hop(1).left()
            k.hd.hop(2).arrived()
            k.hd.hop(2).left()
            k.hd.cross(1).arrived()
            k.hd.cross(1).left()
            k.hd.when_inner(k.hd.cross(2).arrived)
            k.hd.when_inner(k.hd.cross(2).left)

        k3 = run(
            functools.partial(product_body, forward_block, None, ("z", "y", "x", "c"), n, mid_rows, after, begin, end),
            {
                **low_ins(ctx, wo, in_out),
                "x": (xs, WHOLE),
                "bias": (outb, WHOLE),
                "low_out": (out_out, WHOLE),
                "gain": (gains[1:2], WHOLE),
                "shift": (shifts[1:2], WHOLE),
                **ins,
            },
            {
                "mid": (sds(row2, F32), WHOLE),
                "h": (sds(blocks), ANY),
                "lows": (sds((length, rank)), WHOLE),
                **outs,
            },
            "attn_out",
            scratch={**sum_scratch(dict(hv=pltpu.VMEM(row2, BF16))), **links_scratch(32)},
            alias=alias,
            cid=3,
            flops=2 * length * dl * d,
        )
        mid, h2, lo, wu, wd = k3.mid, k3.h.reshape(length, d), k3.lows, k3.wu, k3.wd
    else:
        lo = group_low(ctx, in_out)
        mid = xs.reshape(own, d).astype(F32) + slow_product(forward_block, ctx, wo, "attn_out") + outb + dot(mine(lo), out_out)
        nh, _ = centre(mid)
        h2 = slow_spread((nh * gains[1] + shifts[1]).astype(BF16))
        mid = mid.reshape(row2)

    def flat(w):
        return w.reshape(n, -1, w.shape[-1])

    up_ins = dict(
        h=(h2, once((length, d))),
        w=(flat(wu), pl.BlockSpec((1, d, unit), lambda i: (i, 0, 0))),
        low_in=(in_up, full((rank, d))),
        low_out=(out_up, cols(rank, unit)),
        bias=(upb, cols(1, unit)),
    )
    up_outs = dict(
        act=(sds((length, fl)), cols(length, unit)),
        slope=(sds((length, fl)), cols(length, unit)),
        lu=(sds((length, rank)), full((length, rank))),
    )
    if fast:
        ins, outs, alias = carried(wd=wd)

        def up_carry(r):
            haul = Haul(Links(r.ss, r.rs), r.wd, n)

            def first():
                meet(n, ("z", "y"))
                haul.hop(3).start()
                haul.when_outer(haul.cross(2).start)
                haul.when_inner(haul.cross(3).start)

            def last():
                haul.hop(3).arrived()
                haul.when_outer(haul.cross(3).start)
                haul.hop(3).left()
                haul.when_outer(haul.cross(2).arrived)
                haul.when_outer(haul.cross(2).left)
                haul.cross(3).arrived()
                haul.cross(3).left()

            up_body(r, first, last)

        k4 = run(up_carry, {**up_ins, **ins}, {**up_outs, **outs}, "up", (n,), links_scratch(9), alias, 4, 2 * length * d * fl)
        wd = k4.wd
    else:
        k4 = run(up_body, up_ins, up_outs, "up", (n,))
    act, slope, lu = k4.act, k4.slope, k4.lu
    wu, wd = flat(wu), flat(wd)

    ft = min(512, fl)
    k5 = run(
        gpre_body,
        dict(
            g=(g, once((length, d))),
            w=(wd, pl.BlockSpec((n, ft, d // n), lambda i: (0, i, 0))),
            slope=(slope, cols(length, ft)),
            act=(act, cols(length, ft)),
            low_out=(out_down, full((rank, d))),
            low_in=(in_down, cols(rank, ft)),
            lu=(lu, full((length, rank))),
        ),
        dict(
            gpre=(sds((length, fl)), cols(length, ft)),
            gld=(sds((length, rank)), full((length, rank))),
            tin=(sds((rank, fl)), cols(rank, ft)),
            tout=(sds((rank, fl)), cols(rank, ft)),
        ),
        "gpre",
        (fl // ft,),
        flops=2 * length * d * fl,
    )
    gpre = k5.gpre

    def spread_begin(r, links):
        return Spread(links, r.hv, r.h, r.lh)

    def spread_after(r, k, p):
        k.start(p)

    def spread_end(r, k):
        k.relay(0)
        k.relay(1)
        k.finish()

    term_ins = lambda v: dict(full=(quarter(v), WHOLE))
    term_outs = lambda low: dict(
        lows=(sds((length, low.shape[0])), WHOLE), term=(sds((low.shape[0], dl)), WHOLE)
    )
    if fast:
        k6 = run(
            functools.partial(product_body, backward_block, low_term, ("x", "c"), n, gmid_rows, spread_after, spread_begin, spread_end),
            {
                **low_ins(gpre, wu, out_up),
                "mid": (mid, WHOLE),
                "g": (gs, WHOLE),
                "low_in": (in_up, WHOLE),
                "gain": (gains[1:2], WHOLE),
                **term_ins(h2),
            },
            {"gmid": (sds(row2, F32), WHOLE), "h": (sds(blocks), ANY), **term_outs(out_up)},
            "gmid",
            scratch={**sum_scratch(dict(hv=pltpu.VMEM(row2, BF16))), **links_scratch(16)},
            cid=5,
            flops=2 * length * d * fl,
        )
        gmid, gattn, t_in_up = k6.gmid, k6.h.reshape(length, d), k6.term
    else:
        glu = group_low(gpre, out_up)
        gh = slow_product(backward_block, gpre, wu, "gmid") + dot(mine(glu), in_up)
        gmid = gs.reshape(own, d).astype(F32) + norm_back(mid.reshape(own, d), gh, gains[1])
        gattn = slow_spread(gmid.astype(BF16))
        t_in_up = slow_term(glu, quarter(h2))

    def undeal_begin(r, links):
        return None

    def undeal_end(r, k):
        back = Undeal(r.dsend, r.drecv, 0, r.ov, r.back, *plan)
        back.start()
        back.arrived()
        back.left()

    undeal_scratch = dict(
        ov=pltpu.VMEM(row2, BF16), dsend=pltpu.SemaphoreType.DMA((2,)), drecv=pltpu.SemaphoreType.DMA((2,))
    )
    if fast:
        k7 = run(
            functools.partial(product_body, forward_block, low_term, ("plane", "x"), n, out_rows, None, undeal_begin, undeal_end),
            {
                **low_ins(act, wd, in_down),
                "mid": (mid, WHOLE),
                "bias": (downb, WHOLE),
                "low_out": (out_down, WHOLE),
                **term_ins(g),
            },
            {"back": (sds(inputs.shape), ANY), **term_outs(in_down)},
            "outputs",
            scratch={**sum_scratch(undeal_scratch), **links_scratch(8)},
            cid=6,
            flops=2 * length * d * fl,
        )
        outputs, t_out_down = k7.back, k7.term
    else:
        ld = group_low(act, in_down)
        out = mid.reshape(own, d) + slow_product(forward_block, act, wd, "outputs") + downb + dot(mine(ld), out_down)
        outputs = slow_undeal(out.astype(BF16))
        t_out_down = slow_term(ld, quarter(g))

    k8 = run(
        functools.partial(gctx_body, lambda: lax.axis_index("x") * 2 + lax.axis_index("c")),
        dict(
            g=(gattn, WHOLE),
            w=(wo, WHOLE),
            low_out=(out_out, WHOLE),
            low_in=(in_out, WHOLE),
            ctx=(ctx, WHOLE),
            lo=(lo, WHOLE),
        ),
        dict(
            gctx=(sds((length, dl)), WHOLE),
            tin=(sds((rank, dl)), WHOLE),
            tout=(sds((rank, dl)), WHOLE),
        ),
        "gctx",
        scratch=dict(glo=pltpu.VMEM((length, rank), BF16)),
        flops=2 * length * d * dl,
    )
    early = lax.all_gather(jnp.concatenate([k5.tout, k5.tin, k8.tin, t_in_up, k8.tout, t_out_down], 1), everyone)
    k9 = run(
        functools.partial(attend_back_body, *setup),
        {**att_ins, "g": (k8.gctx, head_cols(0)), "lq": (lq, full((length, 3 * rank)))},
        dict(
            out=(sds((length, 3 * dl)), full((length, 3 * dl))),
            terms=(sds((3, rank, dl)), pl.BlockSpec((3, rank, hd), lambda i: (0, 0, i))),
        ),
        "attend_back",
        (heads,),
        {
            **head_scratch(("qn", "kn", "vn", "gn")),
            "ks": pltpu.VMEM((length, hd), F32),
            "vs": pltpu.VMEM((length, hd), F32),
        },
        flops=5 * att_flops // 2,
    )
    middle = lax.all_gather(k9.terms.reshape(3 * rank, dl), everyone)
    if fast:
        k10 = run(
            functools.partial(product_body, backward_block, low_term, ("plane", "x"), n, final_rows, None, undeal_begin, undeal_end),
            {
                **low_ins(k9.out, wq, ao),
                "x": (xs, WHOLE),
                "gmid": (gmid, WHOLE),
                "low_in": (in_qkv, WHOLE),
                "gain": (gains[0:1], WHOLE),
                **term_ins(h1),
            },
            {"back": (sds(inputs.shape), ANY), **term_outs(ao)},
            "input_grad",
            scratch={**sum_scratch(undeal_scratch), **links_scratch(8)},
            cid=7,
            flops=2 * length * d * 3 * dl,
        )
        input_grad, t_in_qkv = k10.back.astype(F32), k10.term
    else:
        glq = group_low(k9.out, ao)
        gh = slow_product(backward_block, k9.out, wq, "input_grad") + dot(mine(glq), in_qkv)
        gx = gmid + norm_back(xs.reshape(own, d).astype(F32), gh, gains[0])
        input_grad = slow_undeal(gx.astype(BF16)).astype(F32)
        t_in_qkv = slow_term(glq, quarter(h1))
    late = lax.all_gather(t_in_qkv, everyone)

    def by_seq(v):
        return v.reshape((seqs, group) + v.shape[1:])

    def one(height, width):
        return sds((na, height, width), F32), pl.BlockSpec((1, height, width), lambda e: (e, 0, 0))

    k11 = run(
        functools.partial(add_up_body, unit),
        dict(
            index=(adapter_index, pl.BlockSpec(memory_space=pltpu.SMEM)),
            early=(by_seq(early), WHOLE),
            middle=(by_seq(middle), WHOLE),
            late=(by_seq(late), WHOLE),
        ),
        dict(
            inq=one(3 * rank, d),
            outq=one(3 * rank, d),
            ino=one(rank, d),
            outo=one(rank, d),
            inu=one(rank, d),
            outu=one(rank, ff),
            ind=one(rank, ff),
            outd=one(rank, d),
        ),
        "add_up",
        (na,),
    )

    def turn(v):
        return jnp.swapaxes(v, 1, 2)

    return (
        outputs,
        input_grad,
        turn(k11.inq),
        k11.outq.reshape(na, 3, rank, d),
        turn(k11.ino),
        k11.outo,
        turn(k11.inu),
        k11.outu,
        turn(k11.ind),
        k11.outd,
    )


def solution(mesh):
    act = P(("y", "c"), None, ("z", "x"), None)
    weight = P(None, ("z", "x"))
    ins = (act, P(), P(), weight, P(), weight, P(), weight, P(), weight) + (P(),) * 10 + (act,)

    def program(*arrays):
        ndp, nf = mesh.devices.shape
        ny = ndp // 2
        n = arrays[11].shape[0] // ny
        grid = Mesh(mesh.devices.reshape(ny, 2, n, nf // n), ("y", "c", "z", "x"))
        return jax.shard_map(
            shards,
            mesh=grid,
            in_specs=ins,
            out_specs=(act, act) + (P(),) * 8,
            check_vma=False,
        )(*arrays)

    return program
```

```python
import functools
from types import SimpleNamespace

import jax
import jax.numpy as jnp
from jax import lax
from jax.experimental import pallas as pl
from jax.experimental.pallas import tpu as pltpu
from jax.sharding import Mesh
from jax.sharding import PartitionSpec as P

H = 16
EPS = 1e-05
MASKED = -1e30
F32 = jnp.float32
BF16 = jnp.bfloat16
MESH = pl.DeviceIdType.MESH
ANY = pl.BlockSpec(memory_space=pl.ANY)
WHOLE = pl.BlockSpec(memory_space=pltpu.VMEM)
ROWS = 32
TILE = 256


def nn(a, b):
    return jnp.dot(a, b, preferred_element_type=F32)


def nt(a, b):
    return lax.dot_general(a, b, (((1,), (1,)), ((), ())), preferred_element_type=F32)


def tn(a, b):
    return lax.dot_general(a, b, (((0,), (0,)), ((), ())), preferred_element_type=F32)


def centre(v):
    c = v - jnp.mean(v, -1, keepdims=True)
    rstd = lax.rsqrt(jnp.mean(c * c, -1, keepdims=True) + EPS)
    return c * rstd, rstd


def norm_back(v, grad, gain):
    nh, rstd = centre(v)
    e = gain * grad
    return rstd * (e - jnp.mean(e, -1, keepdims=True) - nh * jnp.mean(nh * e, -1, keepdims=True))


def sds(shape, dtype=BF16):
    return jax.ShapeDtypeStruct(shape, dtype)


def full(shape):
    return pl.BlockSpec(shape, lambda *_: (0,) * len(shape))


def once(shape):
    return pl.BlockSpec(shape, lambda *_: (0,) * len(shape), pipeline_mode=pl.Buffered(1))


def cols(height, tile):
    return pl.BlockSpec((height, tile), lambda i: (0, i))


def run(body, ins, outs, name, grid=(), scratch=None, alias=(), cid=None, flops=0):
    scratch = scratch or {}
    names = list(ins) + list(outs) + list(scratch)

    def kernel(*refs):
        body(SimpleNamespace(**dict(zip(names, refs))))

    params = pltpu.CompilerParams(collective_id=cid, has_side_effects=True) if cid is not None else pltpu.CompilerParams()
    result = pl.pallas_call(
        kernel,
        grid=grid,
        in_specs=[s for _, s in ins.values()],
        out_specs=[s for _, s in outs.values()],
        out_shape=[a for a, _ in outs.values()],
        scratch_shapes=list(scratch.values()),
        input_output_aliases={list(ins).index(a): list(outs).index(b) for a, b in alias},
        compiler_params=params,
        cost_estimate=pl.CostEstimate(flops=flops, bytes_accessed=0, transcendentals=0),
        name=name,
    )(*[a for a, _ in ins.values()])
    return SimpleNamespace(**dict(zip(outs, result)))


def row_loop(count, tile, step):
    @pl.loop(0, count // tile)
    def _(r):
        step(pl.ds(pl.multiple_of(r * tile, tile), tile))


def place():
    return tuple(lax.axis_index(a) for a in ("y", "c", "z", "x"))


def meet(n, axes):
    sem = pltpu.get_barrier_semaphore()
    y, c, z, x = place()
    here = {"y": y, "c": c, "x": x}
    pairs = [a for a in axes if a != "z"]
    for a in pairs:
        pl.semaphore_signal(sem, inc=1, device_id={b: 1 - here[b] for b in a}, device_id_type=MESH)
    if "z" in axes:

        @pl.when(z > 0)
        def _():
            pl.semaphore_signal(sem, inc=1, device_id={"z": z - 1}, device_id_type=MESH)

        @pl.when(z < n - 1)
        def _():
            pl.semaphore_signal(sem, inc=1, device_id={"z": z + 1}, device_id_type=MESH)

    count = len(pairs)
    if "z" in axes:
        count += (z + n - 1) // n + (2 * n - 2 - z) // n
    pl.semaphore_wait(sem, count)


def ref(base, *index):
    return lambda: base.at[index] if index else base


def maybe(cond, fn):
    if cond is True:
        fn()
    else:
        pl.when(cond)(fn)


class Sent:
    def __init__(self, links, src, dst, got, where, out_ok=True, in_ok=True):
        k = links.count
        links.count += 1

        def make(src, dst):
            return pltpu.make_async_remote_copy(
                src_ref=src,
                dst_ref=dst,
                send_sem=links.ss.at[k],
                recv_sem=links.rs.at[k],
                device_id=where,
                device_id_type=MESH,
            )

        self.out, self.into = (lambda: make(src(), dst())), (lambda: make(got(), got()))
        self.out_ok, self.in_ok = out_ok, in_ok

    def start(self):
        maybe(self.out_ok, lambda: self.out().start())

    def arrived(self):
        maybe(self.in_ok, lambda: self.into().wait_recv())

    def left(self):
        maybe(self.out_ok, lambda: self.out().wait_send())


class Links:
    def __init__(self, ss, rs):
        self.ss, self.rs, self.count = ss, rs, 0


class Group:
    def __init__(self, copies):
        self.copies = copies

    def start(self):
        for s in self.copies:
            s.start()

    def arrived(self):
        for s in self.copies:
            s.arrived()

    def left(self):
        for s in self.copies:
            s.left()


class Haul:
    def __init__(self, links, w, n, parts=None, chunk=None):
        y, c, z, x = place()
        self.hops = []

        def spot(slot, side):
            return w.at[slot, side] if chunk is None else w.at[slot, side, chunk]

        for t in range(1, n):
            spots = parts if t == 1 and parts else [(None, lambda ref: ref)]
            hop = []
            for src, cut in spots:

                def at(slot, cut=cut):
                    return lambda: cut(spot(slot, y))

                def source(slot, src=src, cut=cut):
                    return (lambda: src(y)) if src else (lambda: cut(spot(slot, y)))

                up_ok = jnp.logical_and(z >= t - 1, z < n - 1)
                down_ok = jnp.logical_and(z + t <= n, z >= 1)
                hop.append(Sent(links, source(z - t + 1), at(z - t + 1), at(z - t), {"z": z + 1}, up_ok, z >= t))
                hop.append(Sent(links, source(z + t - 1), at(z + t - 1), at(z + t), {"z": z - 1}, down_ok, z + t <= n - 1))
            self.hops.append(hop)
        self.across = []
        for slot in (z + 1 - 2 * (z % 2), 2 - z // 2, 3 * (1 - z // 2)):

            def mine(slot=slot):
                return spot(slot, y)

            def other(slot=slot):
                return spot(slot, 1 - y)

            self.across.append(Sent(links, mine, mine, other, {"y": 1 - y}))

    def hop(self, t):
        return Group(self.hops[t - 1])

    def cross(self, j):
        return self.across[j - 1]


class Share:
    def __init__(self, links, mine, out, sem, n):
        y, c, z, x = place()
        self.n = n
        self.local = pltpu.make_async_copy(mine, out.at[c, y, z, x], sem)
        self.sx = Sent(links, lambda: mine, ref(out, c, y, z, x), ref(out, c, y, z, 1 - x), {"x": 1 - x})
        self.sy = Sent(links, ref(out, c, y, z), ref(out, c, y, z), ref(out, c, 1 - y, z), {"y": 1 - y})
        self.sc = Sent(links, ref(out, c), ref(out, c), ref(out, 1 - c), {"c": 1 - c})
        self.hops = []
        for t in range(1, n):

            def at(slot):
                return lambda: out.at[c, :, slot]

            up_ok = jnp.logical_and(z >= t - 1, z < n - 1)
            down_ok = jnp.logical_and(z + t <= n, z >= 1)
            up = Sent(links, at(z - t + 1), at(z - t + 1), at(z - t), {"z": z + 1}, up_ok, z >= t)
            down = Sent(links, at(z + t - 1), at(z + t - 1), at(z + t), {"z": z - 1}, down_ok, z + t <= n - 1)
            self.hops.append(Group([up, down]))

    def start(self):
        self.local.start()
        self.sx.start()

    def step_y(self):
        self.local.wait()
        self.sx.arrived()
        self.sy.start()

    def step_z(self, t):
        if t == 1:
            self.sy.arrived()
        else:
            self.hops[t - 2].arrived()
        self.hops[t - 1].start()

    def step_c(self):
        self.hops[-1].arrived()
        self.sc.start()

    def finish(self):
        self.sc.arrived()
        for s in [self.sx, self.sy, self.sc] + self.hops:
            s.left()


class Spread:
    def __init__(self, links, mine, out, local, count=2):
        y, c, z, x = place()
        me, side, sis, far = c * 2 + x, c * 2 + 1 - x, (1 - c) * 2 + x, (1 - c) * 2 + 1 - x
        self.local = [pltpu.make_async_copy(mine.at[p], out.at[me, p], local.at[p]) for p in range(count)]

        def ref(base, *index):
            return lambda: base.at[index]

        self.xs = [Sent(links, ref(mine, p), ref(out, me, p), ref(out, side, p), {"x": 1 - x}) for p in range(count)]
        self.cs = [Sent(links, ref(mine, p), ref(out, me, p), ref(out, sis, p), {"c": 1 - c}) for p in range(count)]
        self.fs = [Sent(links, ref(out, side, p), ref(out, side, p), ref(out, far, p), {"c": 1 - c}) for p in range(count)]

    def start(self, p):
        self.xs[p].start()
        self.cs[p].start()
        self.local[p].start()

    def relay(self, p):
        self.xs[p].arrived()
        self.fs[p].start()

    def finish(self):
        for p in range(len(self.cs)):
            self.cs[p].arrived()
            self.fs[p].arrived()
            self.local[p].wait()
            for s in (self.xs[p], self.cs[p], self.fs[p]):
                s.left()


class Deal:
    def __init__(self, dsend, drecv, base, src, land, n, zb, per, mb):
        y, c, z, x = place()
        h, zz = z // zb, z % zb
        p = zz % 2
        self.moves = []
        for m in range(mb):
            tc, tz = zz // 2, (c * mb + m) * per + h
            away = jnp.logical_or(tc != c, tz != z)
            far = pltpu.make_async_remote_copy(
                src_ref=src.at[0, m],
                dst_ref=land.at[p],
                send_sem=dsend.at[base + m],
                recv_sem=drecv.at[base + p],
                device_id={"c": tc, "z": tz},
                device_id_type=MESH,
            )
            near = pltpu.make_async_copy(src.at[0, m], land.at[p], drecv.at[base + p])
            self.moves.append((away, far, near))
        self.gets = []
        for q in range(2):
            sz = (z % per) * zb + 2 * c + q
            away = jnp.logical_or(z // (per * mb) != c, sz != z)
            m = (z // per) % mb
            far = pltpu.make_async_remote_copy(
                src_ref=land.at[q],
                dst_ref=land.at[q],
                send_sem=dsend.at[base + q],
                recv_sem=drecv.at[base + q],
                device_id={"c": z // (per * mb), "z": sz},
                device_id_type=MESH,
            )
            near = pltpu.make_async_copy(src.at[0, m], land.at[q], drecv.at[base + q])
            self.gets.append((away, far, near))

    def start(self):
        for away, far, near in self.moves:
            pl.when(away)(lambda far=far: far.start())
            pl.when(jnp.logical_not(away))(lambda near=near: near.start())

    def arrived(self):
        for away, far, near in self.gets:
            pl.when(away)(lambda far=far: far.wait_recv())
            pl.when(jnp.logical_not(away))(lambda near=near: near.wait())

    def left(self):
        for away, far, near in self.moves:
            pl.when(away)(lambda far=far: far.wait_send())


class Undeal:
    def __init__(self, dsend, drecv, base, mine, out, n, zb, per, mb, pieces=1):
        y, c, z, x = place()
        m = (z // per) % mb
        self.pieces = pieces
        step = mine.shape[1] // pieces
        self.moves = []
        for p in range(2):
            tc, tz = z // (per * mb), (z % per) * zb + 2 * c + p
            away = jnp.logical_or(tc != c, tz != z)
            for s in range(pieces):
                at = pl.ds(s * step, step)
                far = pltpu.make_async_remote_copy(
                    src_ref=mine.at[p, at],
                    dst_ref=out.at[0, m, at],
                    send_sem=dsend.at[base + p * pieces + s],
                    recv_sem=drecv.at[base + m * pieces + s],
                    device_id={"c": tc, "z": tz},
                    device_id_type=MESH,
                )
                near = pltpu.make_async_copy(mine.at[p, at], out.at[0, m, at], drecv.at[base + m * pieces + s])
                self.moves.append((away, far, near))
        self.gets = []
        h, zz = z // zb, z % zb
        self.half = zz % 2
        for q in range(mb):
            sc, sz = zz // 2, (c * mb + q) * per + h
            away = jnp.logical_or(sc != c, sz != z)
            for s in range(pieces):
                at = pl.ds(s * step, step)
                far = pltpu.make_async_remote_copy(
                    src_ref=out.at[0, q, at],
                    dst_ref=out.at[0, q, at],
                    send_sem=dsend.at[base + q * pieces + s],
                    recv_sem=drecv.at[base + q * pieces + s],
                    device_id={"c": sc, "z": sz},
                    device_id_type=MESH,
                )
                near = pltpu.make_async_copy(mine.at[zz % 2, at], out.at[0, q, at], drecv.at[base + q * pieces + s])
                self.gets.append((away, far, near))

    def start(self, p, s=0):
        away, far, near = self.moves[p * self.pieces + s]
        pl.when(away)(lambda: far.start())
        pl.when(jnp.logical_not(away))(lambda: near.start())

    def arrived(self, p):
        for away, far, near in self.gets:
            pl.when(jnp.logical_and(self.half == p, away))(lambda far=far: far.wait_recv())
            pl.when(jnp.logical_and(self.half == p, jnp.logical_not(away)))(lambda near=near: near.wait())

    def left(self, p):
        for s in range(self.pieces):
            away, far, near = self.moves[p * self.pieces + s]
            pl.when(away)(lambda far=far: far.wait_send())


def crowd(n, axes=()):
    sem = pltpu.get_barrier_semaphore()
    y, c, z, x = place()
    here = {"y": y, "x": x}
    for cc in range(2):
        for zz in range(n):

            @pl.when(jnp.logical_or(c != cc, z != zz))
            def _(cc=cc, zz=zz):
                pl.semaphore_signal(sem, inc=1, device_id={"c": cc, "z": zz}, device_id_type=MESH)

    for a in axes:
        pl.semaphore_signal(sem, inc=1, device_id={a: 1 - here[a]}, device_id_type=MESH)
    pl.semaphore_wait(sem, 2 * n - 1 + len(axes))


def links_scratch(count):
    return {"ss": pltpu.SemaphoreType.DMA((count,)), "rs": pltpu.SemaphoreType.DMA((count,))}


class ShareZ:
    def __init__(self, links, mine, out, sem, n):
        y, c, z, x = place()
        self.local = pltpu.make_async_copy(mine, out.at[c, y, z, x], sem)
        self.sy = Sent(links, ref(out, c, y, slice(None), x), ref(out, c, y, slice(None), x), ref(out, c, 1 - y, slice(None), x), {"y": 1 - y})

        def lane(xx):
            return ref(out, c, slice(None), slice(None), xx)

        self.sx = Sent(links, lane(x), lane(x), lane(1 - x), {"x": 1 - x})
        self.sc = Sent(links, ref(out, c), ref(out, c), ref(out, 1 - c), {"c": 1 - c})
        self.hops = []
        for t in range(1, n):

            def at(slot):
                return lambda: out.at[c, y, slot, x]

            def source(slot):
                return (lambda: mine) if t == 1 else at(slot)

            up_ok = jnp.logical_and(z >= t - 1, z < n - 1)
            down_ok = jnp.logical_and(z + t <= n, z >= 1)
            up = Sent(links, source(z - t + 1), at(z - t + 1), at(z - t), {"z": z + 1}, up_ok, z >= t)
            down = Sent(links, source(z + t - 1), at(z + t - 1), at(z + t), {"z": z - 1}, down_ok, z + t <= n - 1)
            self.hops.append(Group([up, down]))

    def start(self):
        self.local.start()
        self.hops[0].start()

    def step_z(self, t):
        self.hops[t - 2].arrived()
        self.hops[t - 1].start()

    def step_y(self):
        self.local.wait()
        self.hops[-1].arrived()
        self.sy.start()

    def step_x(self):
        self.sy.arrived()
        self.sx.start()

    def step_c(self):
        self.sx.arrived()
        self.sc.start()

    finish = Share.finish


def edges(first, last, between=None):
    if not (first or last or between):
        return lambda: None
    count = pl.num_programs(0)
    if first:
        pl.when(pl.program_id(0) == 0)(first)
    for at, fn in (between or {}).items():
        pl.when(pl.program_id(0) == at)(fn)
    return lambda: pl.when(pl.program_id(0) == count - 1)(last) if last else None


def qkv_body(r, first=None, last=None, between=None):
    close = edges(first, last, between)
    new = pl.program_id(0) == 0

    def step(at):
        @pl.when(new)
        def _():
            r.lq[at, :] = nt(r.h[at, :], r.low_in[...]).astype(BF16)

        acc = nn(r.h[at, :], r.w[0]) + nn(r.lq[at, :], r.low_out[...])
        r.out[at, :] = (acc + r.bias[...]).astype(BF16)

    row_loop(r.h.shape[0], TILE, step)
    close()


def up_body(r, first=None, last=None, between=None):
    close = edges(first, last, between)
    new = pl.program_id(0) == 0

    def step(at):
        @pl.when(new)
        def _():
            r.lu[at, :] = nt(r.h[at, :], r.low_in[...]).astype(BF16)

        pre = nn(r.h[at, :], r.w[0]) + nn(r.lu[at, :], r.low_out[...]) + r.bias[...]
        cdf = 0.5 * (1.0 + lax.erf(pre * (0.5**0.5)))
        pdf = jnp.exp(-0.5 * pre * pre) * 0.3989422804014327
        r.act[at, :] = (pre * cdf).astype(BF16)
        r.slope[at, :] = (cdf + pre * pdf).astype(BF16)

    row_loop(r.h.shape[0], TILE, step)
    close()


def gpre_body(r):
    new = pl.program_id(0) == 0
    parts, nc = r.w.shape[0], r.w.shape[2]

    def step(at):
        @pl.when(new)
        def _():
            r.gld[at, :] = nt(r.g[at, :], r.low_out[...]).astype(BF16)

        acc = nn(r.gld[at, :], r.low_in[...])
        for p in range(parts):
            acc += nt(r.g[at, p * nc : (p + 1) * nc], r.w[p])
        r.gpre[at, :] = (acc * r.slope[at, :].astype(F32)).astype(BF16)

    row_loop(r.g.shape[0], TILE, step)
    r.terms[0] = tn(r.lu[...], r.gpre[...]).astype(BF16)
    r.terms[1] = tn(r.gld[...], r.act[...]).astype(BF16)


def gctx_body(quarter, r):
    parts, nc = r.w.shape[0], r.w.shape[2]
    dl = r.ctx.shape[1]

    def step(at):
        glo = nt(r.ga[at, :], r.low_out[...]).astype(BF16)
        r.glo[at, :] = glo
        acc = nn(glo, r.low_in[...])
        for p in range(parts):
            acc += nt(r.ga[at, p * nc : (p + 1) * nc], r.w[p])
        r.gctx[at, :] = acc.astype(BF16)

    row_loop(r.ga.shape[0], TILE, step)
    mine = pl.ds(pl.multiple_of(quarter() * dl, dl), dl)
    r.terms[0] = tn(r.glo[...], r.ctx[...]).astype(BF16)
    r.terms[1] = r.before[0]
    r.terms[2] = nn(r.lo[...], r.ga[:, mine]).astype(BF16)
    r.terms[3] = r.before[1]


def forward_block(src, w, out, at, ready=None):
    nc = w.shape[2]

    @pl.loop(0, w.shape[0])
    def _(i):
        if ready:
            ready(i)
        out[:, pl.ds(pl.multiple_of(i * nc, nc), nc)] = nn(src[at, :], w[i]).astype(BF16)


def front_block(src, w, out, at, ready=None):
    nc = w.shape[4]

    @pl.loop(0, w.shape[0])
    def _(i):
        if ready:
            ready(i)
        piece = jnp.concatenate([w[i, a, b] for a in range(2) for b in range(w.shape[2])], 0)
        out[:, pl.ds(pl.multiple_of(i * nc, nc), nc)] = nn(src[at, :], piece).astype(BF16)


def forward_part(w, i):
    return w.at[i]


def backward_block(src, w, out, at, ready=None):
    parts, d, nc = w.shape
    dt = min(512, d)

    @pl.loop(0, d // dt)
    def _(i):
        if ready:
            ready(i)
        rows = pl.ds(pl.multiple_of(i * dt, dt), dt)
        acc = nt(src[at, 0:nc], w[0, rows, :])
        for p in range(1, parts):
            acc += nt(src[at, p * nc : (p + 1) * nc], w[p, rows, :])
        out[:, rows] = acc.astype(BF16)


def backward_part(w, i):
    return w.at[:, pl.ds(pl.multiple_of(i * 512, 512), 512), :]


def backward_half(src, w, out, at, ready, init):
    parts, d, nc = w.shape

    @pl.loop(0, d // 512)
    def _(i):
        ready(i)
        rows = pl.ds(pl.multiple_of(i * 512, 512), 512)
        acc = init[at, rows]
        for p in range(parts):
            acc += nt(src[at, p * nc : (p + 1) * nc], w[p, rows, :])
        out[:, rows] = acc.astype(BF16)


def backward_half_from(w, i):
    return w.at[:, 1, pl.ds(pl.multiple_of(i * 512, 512), 512), :]


def forward_half(src, w, out, at, ready, init):
    nc = w.shape[3]

    @pl.loop(0, w.shape[0])
    def _(i):
        ready(i)
        here = pl.ds(pl.multiple_of(i * nc, nc), nc)
        piece = jnp.concatenate([w[i, 0], w[i, 1]], 0)
        out[:, here] = (init[at, here] + nn(src[at, :], piece)).astype(BF16)


def forward_half_from(w, i):
    return w.at[i, :, 1]


def plain_product_body(block, r):
    @pl.loop(0, r.a.shape[0] // TILE)
    def _(t):
        at = pl.ds(pl.multiple_of(t * TILE, TILE), TILE)
        block(r.a, r.w, r.out.at[at, :], at)


class Product:

    def __init__(self, links, block, piece, a, w, av, wv, part, got, sems, base, order=(0, 1), source=None, init=None):
        y, c, z, x = place()
        self.block, self.av, self.wv, self.part, self.got = block, av, wv, part, got
        own = part.shape[1]
        self.own, self.tok = own, own // 2
        self.c, self.x = c, x
        self.here = a is None
        self.load_a = [lambda t=t: pltpu.make_async_copy(a.at[self.rows(t)], av.at[self.rows(t)], sems.at[base + t]) for t in range(4)]
        source = source or piece
        self.load_w = lambda i: pltpu.make_async_copy(source(w, i), piece(wv, i), sems.at[base + 4 + i])
        self.init = init
        if init:
            self.load_init = lambda t: pltpu.make_async_copy(init[0].at[self.rows(t)], init[1].at[self.rows(t)], init[2].at[t])
        self.any_a = lambda t: pltpu.make_async_copy(a.at[self.rows(t)], av.at[self.rows(t)], sems.at[base + t])
        self.send_a = Sent(links, ref(part, 0), ref(got, 0), ref(got, 0), {"c": 1 - c})
        self.send_c = Sent(links, ref(part, 2), ref(got, 1), ref(got, 1), {"c": 1 - c})

        self.order, self.step = order, own // len(order)

        def half(index, p):
            return lambda: got.at[index, pl.ds(p * self.step, self.step)]

        self.send_b = [Sent(links, half(2, p), half(3, p), half(3, p), {"x": 1 - x}) for p in range(len(order))]

    def rows(self, t):
        cc = jnp.where(t % 2 == 0, 1 - self.c, self.c)
        xx = jnp.where(t < 2, 1 - self.x, self.x)
        return pl.ds(pl.multiple_of((cc * 2 + xx) * self.own, self.own), self.own)

    def load(self, first=True):
        if not self.here:
            self.load_a[0]().start()
        for i in range(4):
            self.load_w(i).start()
            if self.init and first:
                self.load_init(i).start()
        if not self.here:
            for t in range(1, 4):
                self.load_a[t]().start()

    def lows(self, sums, table):
        @pl.loop(0, 4)
        def _(t):
            at = self.rows(t)
            if not self.here:
                pl.when(t > 1)(lambda: self.any_a(t).wait())
            sums.put(at, table[...], self.av[at, :])

        sums.over_c.start()

    def go(self, each=None, send_b=True, low=None, ready_a=False, loaded=False):
        part, got = self.part, self.got

        @pl.loop(0, 4)
        def _(t):
            at = self.rows(t)
            if low is None and not ready_a:
                self.any_a(t).wait()
            elif not self.here:
                pl.when(t < 2)(lambda: self.any_a(t).wait())
            if each:
                each(t, at)

            def ready(i):
                pl.when(t == 0)(lambda: self.load_w(i).wait())

            if self.init:
                self.load_init(t).wait()
                self.block(self.av, self.wv, part.at[t], at, ready, self.init[1])
            else:
                self.block(self.av, self.wv, part.at[t], at, None if loaded else ready)

            @pl.when(t == 0)
            def _():
                self.send_a.start()

            @pl.when(t == 1)
            def _():
                self.send_a.arrived()
                for p in self.order:

                    @pl.loop(0, self.step // ROWS)
                    def _(i):
                        at = pl.ds(pl.multiple_of(p * self.step + i * ROWS, ROWS), ROWS)
                        got[2, at, :] = (part[1, at, :].astype(F32) + got[0, at, :].astype(F32)).astype(BF16)

                    if send_b and (p == 0 or low is None):
                        self.send_b[p].start()

                if low is not None:
                    self.lows(*low)

            if low is not None:

                @pl.when(t == 2)
                def _():
                    low[0].second()
                    for s in self.send_b[1:]:
                        s.start()

            @pl.when(t == 2)
            def _():
                self.send_c.start()

    def own_sum(self, at):
        return self.part[3, at, :].astype(F32) + self.got[1, at, :].astype(F32)

    def left(self, send_b=True):
        for s in [self.send_a, self.send_c] + (self.send_b if send_b else []):
            s.left()


class LowSum:
    def __init__(self, links, low1, low2):
        y, c, z, x = place()
        self.low1, self.low2 = low1, low2
        self.over_c = Sent(links, ref(low1, 0), ref(low1, 1), ref(low1, 1), {"c": 1 - c})
        self.over_x = Sent(links, ref(low2, 0), ref(low2, 1), ref(low2, 1), {"x": 1 - x})

    def put(self, at, table, rows):
        self.low1[0, :, at] = nt(table, rows).astype(BF16)

    def second(self):
        self.over_c.arrived()
        self.low2[0] = (self.low1[0].astype(F32) + self.low1[1].astype(F32)).astype(BF16)
        self.over_x.start()

    def total(self):
        self.over_x.arrived()
        return (self.low2[0].astype(F32) + self.low2[1].astype(F32)).astype(BF16)

    def left(self):
        self.over_c.left()
        self.over_x.left()


def own_low(lows, table, p, tok, out):
    y, c, z, x = place()
    at = pl.ds(pl.multiple_of((c * 2 + x) * 2 * tok + p * tok, tok), tok)
    out[...] = tn(lows[:, at], table)


def each_row(tok, p, fn, start=0, count=None):

    @pl.loop(0, (count or tok) // ROWS)
    def _(i):
        at = pl.ds(pl.multiple_of(start + i * ROWS, ROWS), ROWS)
        mine = pl.ds(pl.multiple_of(p * tok + start + i * ROWS, ROWS), ROWS)
        fn(at, mine)


def front_body(n, zb, per, mb, setup, r):
    y, c, z, x = place()
    hd = r.qs.shape[3] // 2
    uc, dc = r.us.shape[3], r.ds.shape[3]
    crowd(n, ("x", "y"))
    links = Links(r.ss, r.rs)
    own = r.part.shape[1]
    tok = own // 2
    heads = r.qkv.shape[1] // (3 * hd)
    nq = r.wq.shape[4]
    length = r.h1v.shape[0] * own
    deal_x = Deal(r.dsend, r.drecv, 0, r.inputs, r.xv, n, zb, per, mb)
    deal_g = Deal(r.dsend, r.drecv, 2, r.cot, r.gv, n, zb, per, mb)
    deal_x.start()

    def lanes(start, size):
        return pl.ds(pl.multiple_of(start, 128), size)

    stage = [
        pltpu.make_async_copy(r.wq_in.at[..., lanes(c * hd, hd)], r.qs.at[..., 0:hd], r.ls.at[0]),
        pltpu.make_async_copy(r.wq_in.at[..., lanes((c + 4) * hd, hd)], r.qs.at[..., hd : 2 * hd], r.ls.at[1]),
        pltpu.make_async_copy(r.wo_in.at[:, :, x, c], r.os, r.ls.at[2]),
        pltpu.make_async_copy(r.wu_in.at[:, :, :, lanes(c * uc, uc)], r.us, r.ls.at[3]),
        pltpu.make_async_copy(r.wd_in.at[:, :, x, c], r.ds, r.ls.at[4]),
    ]
    for s in stage:
        s.start()

    def q_keep(ref):
        return ref.at[..., lanes(hd * x, 2 * hd)]

    def q_got(ref):
        return ref.at[..., lanes(2 * hd * (1 - x), hd)]

    def q_give(ref):
        return ref.at[..., lanes(2 * hd * x, hd)]

    def d_keep(ref):
        return ref.at[..., lanes(dc * x, dc)]

    def d_got(ref):
        return ref.at[..., lanes(dc * (1 - x), dc)]

    side = {"x": 1 - x}
    swap_q = Sent(
        links, lambda: r.wq_in.at[..., lanes((c + 2) * hd, hd)], lambda: q_give(r.wq.at[z]), lambda: q_got(r.wq.at[z]), side
    )
    swap_o = Sent(links, lambda: r.wo_in.at[:, :, 1 - x, c], lambda: d_keep(r.wo.at[z]), lambda: d_got(r.wo.at[z]), side)
    swap_d = Sent(links, lambda: r.wd_in.at[:, :, 1 - x, c], lambda: d_keep(r.wd.at[z]), lambda: d_got(r.wd.at[z]), side)
    swap_q.start()
    swap_o.start()
    haul_q = [Haul(links, r.wq, n, [(lambda y, k=k: r.qs.at[y, k], q_keep), (None, q_got)], k) for k in range(2)]
    haul_o = Haul(links, r.wo, n, [(lambda y: r.os.at[y], d_keep), (None, d_got)])
    spread_1 = Spread(links, r.hv, r.h1, r.lh1)
    for s in stage:
        s.wait()
    hauls = haul_q + [haul_o]
    ones = [haul.hop(1).copies for haul in hauls]
    for one in ones:
        Group(one[:2]).start()
    keep = [
        pltpu.make_async_copy(r.qs, q_keep(r.wq.at[z]), r.ls.at[0]),
        pltpu.make_async_copy(r.os, d_keep(r.wo.at[z]), r.ls.at[1]),
        pltpu.make_async_copy(r.us, r.wu.at[z], r.ls.at[2]),
        pltpu.make_async_copy(r.ds, d_keep(r.wd.at[z]), r.ls.at[3]),
    ]
    for s in keep:
        s.start()
    swap_q.arrived()
    for one in ones[:2]:
        Group(one[2:]).start()
    swap_o.arrived()
    Group(ones[2][2:]).start()

    deal_x.arrived()
    for p in range(2):

        @pl.loop(0, tok // ROWS)
        def _(i):
            at = pl.ds(pl.multiple_of(i * ROWS, ROWS), ROWS)
            v = r.xv[p, at, :]
            r.x[p, at, :] = v
            nh, _ = centre(v.astype(F32))
            h = (nh * r.gain[0:1].astype(F32) + r.shift[0:1].astype(F32)).astype(BF16)
            r.hv[p, at, :] = h

        spread_1.start(p)
    swap_d.start()

    def step(haul, t):
        haul.hop(t).arrived()
        if t < n - 1:
            haul.hop(t + 1).start()
        haul.cross(t).start()

    for haul in hauls:
        step(haul, 1)
    spread_1.relay(0)
    spread_1.relay(1)
    for haul in hauls:
        step(haul, 2)
    hu = [Haul(links, r.wu, n, [(lambda y, k=k: r.us.at[y, k], lambda ref: ref)], k) for k in range(2)]
    hw = [Haul(links, r.wd, n, chunk=k) for k in range(2)]
    hu[0].hop(1).start()
    hu[1].hop(1).start()
    for haul in hauls:
        step(haul, 3)
    for s in keep:
        s.wait()
    spread_1.finish()

    def h1_rows(t):
        return pltpu.make_async_copy(r.h1.at[t], r.h1v.at[t], r.lq1.at[t])

    def wq_part(i):
        return pltpu.make_async_copy(r.wq.at[i], r.wqv.at[i], r.lq2.at[i])

    for t in range(4):
        h1_rows(t).start()
    for haul in hauls:
        for j in (1, 2, 3):
            haul.cross(j).arrived()
    for i in range(n):
        wq_part(i).start()
    product = Product(links, front_block, forward_part, None, r.wo, r.ctx, r.wv, r.part, r.got, r.ls8, 0)
    spread = Spread(links, r.hv2, r.h, r.lh)
    spread_w = Spread(links, r.wv, r.wof, r.lhw, n)
    sums = LowSum(links, r.low1, r.low2)
    product.load()
    for i in range(n):
        product.load_w(i).wait()
        spread_w.start(i)

    def pump_1():
        hu[0].hop(1).arrived()
        hu[0].hop(2).start()
        hu[0].cross(1).start()

    @pl.loop(0, n)
    def _(i):
        pl.when(i == 2)(pump_1)
        wq_part(i).wait()
        at_cols = pl.ds(pl.multiple_of(i * nq, nq), nq)

        @pl.loop(0, 4)
        def _(t):
            at = pl.ds(pl.multiple_of(t * own, own), own)

            @pl.when(i == 0)
            def _():
                h1_rows(t).wait()

            rows = jnp.concatenate([r.h1v[t, 0], r.h1v[t, 1]], 0)

            @pl.when(i == 0)
            def _():
                r.lq[at, :] = nt(rows, r.low_in[...]).astype(BF16)

            piece = jnp.concatenate([r.wqv[i, a, b] for a in range(2) for b in range(2)], 0)
            acc = nn(rows, piece) + nn(r.lq[at, :], r.low_out[:, at_cols])
            r.qkv[at, at_cols] = (acc + r.bias[:, at_cols]).astype(BF16)

    def pump_2():
        hu[1].hop(1).arrived()
        hu[1].hop(2).start()
        hu[1].cross(1).start()
        deal_g.start()

    @pl.loop(0, heads)
    def _(head):
        pl.when(head == 2)(pump_2)
        q, k, v = (r.qkv.at[:, pl.ds(pl.multiple_of((j * heads + head) * hd, hd), hd)] for j in range(3))
        ctx = r.ctx.at[:, pl.ds(pl.multiple_of(head * hd, hd), hd)]
        attend_body(*setup, SimpleNamespace(q=q, k=k, v=v, ctx=ctx, qn=r.qn, kn=r.kn, vn=r.vn))

    def pump_3():
        hu[0].hop(2).arrived()
        hu[0].hop(3).start()
        swap_d.arrived()
        hw[0].hop(1).start()
        hu[0].cross(2).start()

    product.go(lambda t, at: pl.when(t == 3)(pump_3), low=(sums, r.low), loaded=True)
    hu[1].hop(2).arrived()
    hu[1].hop(3).start()
    hu[1].cross(2).start()
    r.lows[...] = sums.total()
    product.send_c.arrived()
    for p in range(2):
        own_low(r.lows, r.low_out2[...], p, tok, r.lowv)
        product.send_b[p].arrived()

        def rows(at, mine, p=p):
            s = product.own_sum(mine) + r.got[3, mine, :].astype(F32)
            mid = r.x[p, at, :].astype(F32) + s + r.bias2[...].astype(F32) + r.lowv[at, :]
            r.mid[p, at, :] = mid
            nh, _ = centre(mid)
            r.hv2[p, at, :] = (nh * r.gain[1:2].astype(F32) + r.shift[1:2].astype(F32)).astype(BF16)

        each_row(tok, p, rows)
        spread.start(p)
        if p == 0:
            hu[0].hop(3).arrived()
            hu[0].cross(3).start()
    hw[0].hop(1).arrived()
    hw[0].hop(2).start()
    hw[0].cross(1).start()
    spread.relay(0)
    hu[1].hop(3).arrived()
    hu[1].cross(3).start()
    spread.relay(1)
    for i in range(n):
        spread_w.relay(i)
    spread.finish()
    spread_w.finish()
    hw[0].hop(2).arrived()
    for j in (1, 2, 3):
        for k in range(2):
            hu[k].cross(j).arrived()
            hu[k].cross(j).left()
            hu[k].hop(j).left()
    hw[0].cross(1).arrived()
    for s in (hw[0].cross(1), hw[0].hop(1), hw[0].hop(2), product, sums):
        s.left()
    deal_g.arrived()
    for p in range(2):
        r.gs[p] = r.gv[p]
    for haul in hauls:
        for j in (1, 2, 3):
            haul.cross(j).left()
            haul.hop(j).left()
    for s in (swap_q, swap_o, swap_d, deal_x, deal_g):
        s.left()


def up_body_fast(n, r):
    y = lax.axis_index("y")
    meet(n, ("z", "y", "x", "c"))
    links = Links(r.ss, r.rs)
    a, b = (Haul(links, r.wd, n, chunk=k) for k in range(2))
    spread = Spread(links, r.gs, r.g4, r.lsp)
    spread.start(0)
    spread.start(1)
    a.hop(3).start()
    b.hop(1).start()
    a.cross(2).start()
    length = r.hv.shape[0]
    own = length // 4
    unit = r.wu.shape[2]

    def h_rows(t):
        at = pl.ds(pl.multiple_of(t * own, own), own)
        return pltpu.make_async_copy(r.h.at[at], r.hv.at[at], r.lh.at[t])

    def g_rows(t):
        at = pl.ds(pl.multiple_of(t * own, own), own)
        return pltpu.make_async_copy(r.g4.at[t], r.gv.at[t], r.lg.at[t])

    def wu_part(i):
        return pltpu.make_async_copy(r.wu.at[i], r.wuv.at[i], r.lu1.at[i])

    def cols_of(i):
        return pl.ds(pl.multiple_of(i * unit, unit), unit)

    def act_out(j):
        return pltpu.make_async_copy(r.actv.at[:, cols_of(2 * j + 1)], r.act.at[:, cols_of(j)], r.lo1.at[j])

    def gpre_out(j):
        return pltpu.make_async_copy(r.gprev.at[:, cols_of(2 * j + 1)], r.gpre.at[:, cols_of(j)], r.lo2.at[j])

    def wd_part(phase, j):
        return pltpu.make_async_copy(r.wd.at[:, j, phase], r.wdv.at[phase, j], r.lw.at[2 * phase + j])

    def keep(t, out, sems):
        at = pl.ds(pl.multiple_of(t * own, own), own)
        return pltpu.make_async_copy(r.stage.at[t % 2], out.at[at], sems.at[t % 2])

    def first_halves(term, out, sems):
        @pl.loop(0, 4)
        def _(t):
            at = pl.ds(pl.multiple_of(t * own, own), own)
            pl.when(t > 1)(lambda: keep(t - 2, out, sems).wait())

            @pl.loop(0, 4)
            def _(i):
                here = pl.ds(pl.multiple_of(i * 512, 512), 512)
                r.stage[t % 2, :, here] = term(at, i, here)

            keep(t, out, sems).start()

        for t in (2, 3):
            keep(t, out, sems).wait()

    def back_term(at, i, here):
        return nt(r.gprev[at, 0:unit], r.wuv[0, here, :]) + nt(r.gprev[at, 2 * unit : 3 * unit], r.wuv[2, here, :])

    def forth_term(at, i, here):
        return nn(r.actv[at, 0:unit], r.wdv[0, 0, i]) + nn(r.actv[at, 2 * unit : 3 * unit], r.wdv[0, 1, i])

    h_rows(0).start()
    wu_part(0).start()
    for t in range(1, 4):
        h_rows(t).start()
    for i in range(1, n):
        wu_part(i).start()

    def pump_1():
        a.hop(3).arrived()
        a.cross(3).start()
        spread.relay(0)

    @pl.loop(0, n)
    def _(i):
        pl.when(i == 3)(pump_1)
        wu_part(i).wait()
        here = cols_of(i)

        @pl.loop(0, 4)
        def _(t):
            at = pl.ds(pl.multiple_of(t * own, own), own)

            @pl.when(i == 0)
            def _():
                h_rows(t).wait()
                r.lu[at, :] = nt(r.hv[at, :], r.low_in[...]).astype(BF16)

            pre = nn(r.hv[at, :], r.wuv[i]) + nn(r.lu[at, :], r.low_out[:, here]) + r.bias[:, here]
            cdf = 0.5 * (1.0 + lax.erf(pre * (0.5**0.5)))
            pdf = jnp.exp(-0.5 * pre * pre) * 0.3989422804014327
            act = (pre * cdf).astype(BF16)
            r.actv[at, here] = act
            r.slopev[at, here] = (cdf + pre * pdf).astype(BF16)
            low = nt(r.low_in2[:, here], act)
            r.ldv[:, at] = jnp.where(i == 0, low, r.ldv[:, at] + low)

        pl.when(i % 2 == 1)(act_out(i // 2).start)

    a.cross(2).arrived()
    b.hop(1).arrived()
    b.hop(2).start()
    b.cross(1).start()
    spread.relay(1)
    spread.finish()
    for t in range(4):
        g_rows(t).start()
    a.cross(3).arrived()
    for j in range(2):
        wd_part(0, j).start()

    @pl.loop(0, 4)
    def _(t):
        at = pl.ds(pl.multiple_of(t * own, own), own)
        g_rows(t).wait()
        for p in range(2):
            half = pl.ds(pl.multiple_of(t * own + p * (own // 2), own // 2), own // 2)
            r.gld[half, :] = nt(r.gv[t, p], r.low_out2[...]).astype(BF16)

    @pl.loop(0, 4)
    def _(k):
        phase = k // 2
        j = (k + y) % 2

        @pl.when(k == 2)
        def _():
            b.hop(2).arrived()
            b.hop(3).start()
            b.cross(2).start()
            first_halves(back_term, r.acc1, r.lk1)
            b.hop(3).arrived()
            b.cross(3).start()
            wd_part(1, j).start()

        @pl.when(k == 3)
        def _():
            first_halves(forth_term, r.acc2, r.lk2)
            for t in (1, 2, 3):
                b.cross(t).arrived()
            wd_part(1, j).start()

        wd_part(phase, j).wait()
        here = cols_of(2 * j + phase)
        nc = r.wdv.shape[4]

        @pl.loop(0, 4)
        def _(t):
            at = pl.ds(pl.multiple_of(t * own, own), own)
            rows = jnp.concatenate([r.gv[t, 0], r.gv[t, 1]], 0)
            acc = nn(r.gld[at, :], r.low_in2[:, here])
            for p in range(n):
                acc += nt(rows[:, p * nc : (p + 1) * nc], r.wdv[phase, j, p])
            gpre = (acc * r.slopev[at, here].astype(F32)).astype(BF16)
            r.gprev[at, here] = gpre
            low = nt(r.low_out[:, here], gpre)
            r.gluv[:, at] = jnp.where(k == 0, low, r.gluv[:, at] + low)

        pl.when(phase == 1)(gpre_out(j).start)
        r.terms[0, :, here] = tn(r.lu[...], r.gprev[:, here]).astype(BF16)
        r.terms[1, :, here] = tn(r.gld[...], r.actv[:, here]).astype(BF16)

    r.glu_part[...] = r.gluv[...].astype(BF16)
    r.ld_part[...] = r.ldv[...].astype(BF16)
    for j in range(2):
        act_out(j).wait()
        gpre_out(j).wait()
    for s in (a.hop(3), b.hop(1), b.hop(2), b.hop(3), a.cross(2), a.cross(3), b.cross(1), b.cross(2), b.cross(3)):
        s.left()


def own_quarter(source, out, sem):
    y, c, z, x = place()
    dl = out.shape[1]
    return pltpu.make_async_copy(source.at[:, pl.ds(pl.multiple_of((x * 2 + c) * dl, dl), dl)], out, sem)


class Corners:
    def __init__(self, links, mine, land, got):
        y, c, z, x = place()
        self.me = c * 2 + x
        self.peers = [
            (c * 2 + 1 - x, {"x": 1 - x}),
            ((1 - c) * 2 + 1 - x, {"x": 1 - x, "c": 1 - c}),
            ((1 - c) * 2 + x, {"c": 1 - c}),
        ]
        self.copies = [Sent(links, mine(b), land(self.me), got(b), where) for b, where in self.peers]

    def start(self):
        for s in self.copies:
            s.start()

    def arrived(self):
        for s in self.copies:
            s.arrived()

    def left(self):
        for s in self.copies:
            s.left()


def gmid_body(n, r):
    y, c, z, x = place()
    meet(n, ("z", "y", "x", "c", "xc"))
    links = Links(r.ss, r.rs)
    share = Share(links, r.pack, r.shared, r.lsh.at[0], n)
    product = Product(
        links, backward_half, backward_part, r.a, r.w, r.av, r.wv, r.part, r.got, r.ls, 0, (0, 1), backward_half_from, (r.acc1, r.i1, r.li1)
    )
    second = Product(
        links, forward_half, forward_part, r.b, r.v, r.bv, r.vv, r.part2, r.got2, r.ls, 8, (0, 1), forward_half_from, (r.acc2, r.i1, r.li2)
    )
    product.load()
    share.start()
    wof = pltpu.make_async_copy(r.wof, r.wfv, r.lsh.at[3])
    wof.start()
    second.load(False)
    quarters = [own_quarter(r.full, r.fv, r.lsh.at[1]), own_quarter(r.full_b, r.gv, r.lsh.at[2])]
    for q in quarters:
        q.start()
    sums = LowSum(links, r.low1, r.low2)
    sums_b = LowSum(links, r.low1b, r.low2b)
    tok, d = r.hv.shape[1:]
    dl = d // 4
    me = c * 2 + x
    deals = [Corners(links, lambda b, p=p: ref(r.send, p, b), lambda b, p=p: ref(r.gctx, b, p), lambda b, p=p: ref(r.gctx, b, p)) for p in range(2)]
    stay = [pltpu.make_async_copy(r.send.at[p, me], r.gctx.at[me, p], r.lh.at[p]) for p in range(2)]
    glo_deal = Corners(links, lambda b: ref(r.glos, me), lambda b: ref(r.glos, b), lambda b: ref(r.glos, b))
    term_deal = Corners(links, lambda b: ref(r.tsend, b), lambda b: ref(r.tgot, b), lambda b: ref(r.tgot, b))
    r.low1[0] = r.low[...]
    r.low1b[0] = r.low_b[...]
    sums.over_c.start()
    sums_b.over_c.start()

    def early_sums(t, at):
        @pl.when(t == 1)
        def _():
            sums.second()
            sums_b.second()

        pl.when(t == 2)(share.step_y)

    product.go(early_sums)
    for t in range(4):
        second.load_init(t).start()
    r.glu[...] = sums.total()

    def own_rows(p):
        own_low(r.glu, r.low_in[...], p, tok, r.lowv)
        product.send_b[p].arrived()

        def rows(at, mine):
            gh = product.own_sum(mine) + r.got[3, mine, :].astype(F32) + r.lowv[at, :]
            gmid = r.g[p, at, :].astype(F32) + norm_back(r.mid[p, at, :], gh, r.gain[1:2].astype(F32))
            r.gmid[p, at, :] = gmid
            r.hv[p, at, :] = gmid.astype(BF16)

        each_row(tok, p, rows)
        r.glos[me, :, p * tok : (p + 1) * tok] = nt(r.out_out[...], r.hv[p]).astype(BF16)
        if p == 0:
            wof.wait()

        @pl.loop(0, 4)
        def _(k):
            b = jnp.where(k == 0, c * 2 + 1 - x, jnp.where(k == 1, (1 - c) * 2 + 1 - x, jnp.where(k == 2, (1 - c) * 2 + x, me)))
            acc = tn(r.glos[me, :, p * tok : (p + 1) * tok], r.in_all[b])
            nc = r.wfv.shape[2]
            for q in range(n):
                acc += nt(r.hv[p, :, q * nc : (q + 1) * nc], r.wfv[b, q * dl : (q + 1) * dl, :])
            r.send[p, b] = acc.astype(BF16)
            for i in range(3):
                pl.when(k == i)(deals[p].copies[i].start)
            pl.when(k == 3)(stay[p].start)

    def between(t, at):
        @pl.when(t == 1)
        def _():
            share.step_z(1)

        @pl.when(t == 3)
        def _():
            product.send_c.arrived()
            own_rows(0)
            share.step_z(2)

    second.go(between, False)
    own_rows(1)
    glo_deal.start()
    share.step_z(3)

    for b in range(4):
        cc, xx = divmod(b, 2)
        here = slice((xx * 2 + cc) * dl, (xx * 2 + cc + 1) * dl)
        parts = []
        for p in range(2):
            at = pl.ds(pl.multiple_of(me * 2 * tok + p * tok, tok), tok)
            parts.append(nn(r.lo[:, at], r.hv[p, :, here]))
        r.tsend[b] = (parts[0] + parts[1]).astype(BF16)
    term_deal.start()
    second.send_c.arrived()
    for p in range(2):

        def rows(at, mine, p=p):
            r.sb[p, at, :] = r.got2[2, mine, :]
            r.sd[p, at, :] = second.own_sum(mine)

        each_row(tok, p, rows)
    for q in quarters:
        q.wait()
    r.terms[0] = nn(r.glu[...], r.fv[...]).astype(BF16)
    r.lows[...] = sums_b.total()
    r.terms[1] = nn(r.lows[...], r.gv[...]).astype(BF16)
    glo_deal.arrived()
    r.glo[...] = r.glos[...]
    term_deal.arrived()
    total = r.tsend[me].astype(F32)
    for b, _ in term_deal.peers:
        total += r.tgot[b].astype(F32)
    r.terms[2] = total.astype(BF16)
    share.step_c()
    for p in range(2):
        deals[p].arrived()
        stay[p].wait()
    share.finish()
    second.left(False)
    for s in deals + [glo_deal, term_deal, product, sums, sums_b]:
        s.left()


def back_body(plan, setup, r):
    n = plan[0]
    y, c, z, x = place()
    crowd(n, ("x", "y"))
    links = Links(r.ss, r.rs)
    length, hd = r.qkv.shape[0], r.qn.shape[1]
    heads = r.qkv.shape[1] // (3 * hd)
    own = length // 4
    tok = own // 2
    across = Sent(links, ref(r.sb), ref(r.rb), ref(r.rb), {"x": 1 - x})
    share_m = Share(links, r.terms, r.shared_m, r.lsh.at[0], n)
    share_l = ShareZ(links, r.late, r.shared_l, r.lsh.at[1], n)
    lows = LowSum(links, r.low1, r.low2)
    product = Product(links, backward_block, backward_part, None, r.wq, r.out, r.wqv, r.part, r.got, r.ls, 0, (0, 2, 1, 3))
    leave = Undeal(r.dsend, r.drecv, 0, r.outv, r.outputs, *plan)
    home = Undeal(r.dsend, r.drecv, 2, r.gv, r.back, *plan, 2)
    quarter = own_quarter(r.full, r.fv, r.lsh.at[2])
    pairs = ((r.ctx_in, r.ctx), (r.qkv_in, r.qkv), (r.gctx_in, r.gctx), (r.mid_in, r.mid), (r.sd_in, r.sd))
    pairs += ((r.gmid_in, r.gmid), (r.x_in, r.x))
    loads = [pltpu.make_async_copy(a, b, r.ld8.at[k]) for k, (a, b) in enumerate(pairs)]
    for one in loads[:3]:
        one.start()
    product.load()
    for one in loads[3:]:
        one.start()
    quarter.start()
    loads[0].wait()
    total = nn(r.glo[0], r.ctx[0:own, :])
    for b in range(1, 4):
        total += nn(r.glo[b], r.ctx[b * own : (b + 1) * own, :])
    r.terms[0] = total.astype(BF16)
    r.terms[1] = r.before[0]
    r.terms[2] = r.before[2]
    r.terms[3] = r.before[1]
    share_m.start()
    across.start()
    for one in loads[1:3]:
        one.wait()

    def output(p):
        own_low(r.ld, r.low_down[...], p, tok, r.lowv)

        def rows(at, mine):
            s = r.mid[p, at, :] + r.sd[p, at, :] + r.rb[p, at, :].astype(F32) + r.bias[...].astype(F32)
            r.outv[p, at, :] = (s + r.lowv[at, :]).astype(BF16)

        each_row(tok, p, rows)

    def first_half():
        across.arrived()
        for one in loads[3:5]:
            one.wait()
        output(0)

    polls = (
        ((0, 0), share_m.step_y),
        ((1, 0), lambda: share_m.step_z(1)),
        ((3, 0), lambda: share_m.step_z(2)),
    )

    @pl.loop(0, heads)
    def _(head):
        def poll(block):
            for at, fn in polls:
                if at[1] == block:
                    pl.when(head == at[0])(fn)

        attend_back_body(*setup, r, head, heads, poll)

    row_loop(length, TILE, lambda at: lows.put(at, r.ao[...], r.out[at, :]))
    lows.over_c.start()

    def between(t, at):
        pl.when(t == 1)(lows.second)

        @pl.when(t == 2)
        def _():
            share_m.step_z(3)
            first_half()

        @pl.when(t == 3)
        def _():
            r.glq[...] = lows.total()
            quarter.wait()
            r.late[1] = nn(r.glq[...], r.fv[...]).astype(BF16)
            share_l.start()
            output(1)

    product.go(between, ready_a=True)
    share_l.step_z(2)
    product.send_c.arrived()
    for one in loads[5:]:
        one.wait()
    quick = tok // 2

    for p in range(2):
        own_low(r.glq, r.low_back[...], p, tok, r.lowb.at[p])

    def last_hop():
        share_l.step_z(3)
        leave.start(0)
        leave.start(1)

    steps = [last_hop, lambda: None, share_l.step_y, share_l.step_x]
    for piece, step in zip(product.order, steps):
        p, k = divmod(piece, 2)

        def rows(at, mine, p=p):
            gh = product.own_sum(mine) + r.got[3, mine, :].astype(F32) + r.lowb[p, at, :]
            v = r.x[p, at, :].astype(F32)
            r.gv[p, at, :] = (r.gmid[p, at, :] + norm_back(v, gh, r.gain[0:1].astype(F32))).astype(BF16)

        product.send_b[piece].arrived()
        each_row(tok, p, rows, k * quick, quick)
        home.start(p, k)
        step()
    share_m.step_c()
    share_l.step_c()
    for p in range(2):
        leave.arrived(p)
        leave.left(p)
    for p in range(2):
        home.arrived(p)
        home.left(p)
    share_m.finish()
    share_l.finish()
    product.left()
    across.left()
    lows.left()


def select_body(group, heads, n, dev, chosen, *refs):
    names = ("in_qkv", "out_qkv", "in_out", "out_out", "in_up", "out_up", "in_down", "out_down", "qv", "up")
    outs = ("in_qkv", "ao", "in_all", "in_out", "out_out", "in_up", "out_up", "in_down", "out_down", "qkv_bias", "up_bias")
    t = SimpleNamespace(**dict(zip(names, refs)))
    o = SimpleNamespace(**dict(zip(outs, refs[len(names) :])))
    q = dev()
    rank, d = t.out_out.shape[1:]
    hd = d // H
    dl = heads * hd
    fl = o.out_up.shape[1]
    unit = fl // n

    def spot(i, size):
        return pl.ds(pl.multiple_of((i * group + q) * size, size), size)

    o.in_qkv[...] = t.in_qkv[0]
    o.out_out[...] = t.out_out[0]
    o.in_up[...] = t.in_up[0]
    o.out_down[...] = t.out_down[0]
    o.ao[...] = jnp.zeros_like(o.ao)
    for b in range(group):
        cc, xx = divmod(b, group // 2)
        for i in range(heads):
            at = (i * group + xx * 2 + cc) * hd
            o.in_all[b, :, i * hd : (i + 1) * hd] = t.in_out[0, :, at : at + hd]
    for i in range(heads):
        here = slice(i * hd, (i + 1) * hd)
        o.in_out[:, here] = t.in_out[0, :, spot(i, hd)]
        for j in range(3):
            o.ao[j * rank : (j + 1) * rank, j * dl + i * hd : j * dl + (i + 1) * hd] = t.out_qkv[0, j, :, spot(i, hd)]
        o.qkv_bias[:, here] = t.qv[0:1, spot(i, hd)].astype(F32)
        o.qkv_bias[:, dl + i * hd : dl + (i + 1) * hd] = jnp.zeros((1, hd), F32)
        o.qkv_bias[:, 2 * dl + i * hd : 2 * dl + (i + 1) * hd] = t.qv[1:2, spot(i, hd)].astype(F32)
    for i in range(n):
        here = slice(i * unit, (i + 1) * unit)
        o.out_up[:, here] = t.out_up[0, :, spot(i, unit)]
        o.in_down[:, here] = t.in_down[0, :, spot(i, unit)]
        o.up_bias[:, here] = t.up[0:1, spot(i, unit)].astype(F32)


def places(length, tok, nx):
    spots = []
    for b in range(length // tok):
        lead, xx = divmod(b, nx)
        cc, p = divmod(lead, 2)
        spots.append(((cc * nx + xx) * 2 + p) * tok)
    return spots


def in_order(ref, out, spots, tok):
    for b, at in enumerate(spots):
        out[b * tok : (b + 1) * tok, :] = ref[at : at + tok, :]


def softmax_block(q, k, start, scale):
    s = nt(q, k) * scale
    r = lax.broadcasted_iota(jnp.int32, s.shape, 0) + start
    c = lax.broadcasted_iota(jnp.int32, s.shape, 1)
    s = jnp.where(r >= c, s, MASKED)
    p = jnp.exp(s - jnp.max(s, -1, keepdims=True))
    return p * (1.0 / jnp.sum(p, -1, keepdims=True))


def attend_body(bq, tok, spots, scale, r, first=None, last=None):
    close = edges(first, last)
    length = r.q.shape[0]
    for ref, out in ((r.q, r.qn), (r.k, r.kn), (r.v, r.vn)):
        in_order(ref, out, spots, tok)
    for start in range(0, length, bq):
        end = start + bq
        p = softmax_block(r.qn[start:end, :], r.kn[:end, :], start, scale)
        ctx = nn(p.astype(BF16), r.vn[:end, :]).astype(BF16)
        for i in range(bq // tok):
            at = spots[start // tok + i]
            r.ctx[at : at + tok, :] = ctx[i * tok : (i + 1) * tok]
    close()


def attend_back_body(bq, tok, spots, scale, r, head, heads, poll=None):
    length, hd = r.qkv.shape[0], r.qn.shape[1]
    own_heads = pl.ds(pl.multiple_of(head * hd, hd), hd)
    rank = r.lq.shape[1] // 3

    def third(base, i):
        return base.at[:, pl.ds(pl.multiple_of((i * heads + head) * hd, hd), hd)]

    gq, gk, gv = (third(r.out, i) for i in range(3))
    for base, out in ((third(r.qkv, 0), r.qn), (third(r.qkv, 1), r.kn), (third(r.qkv, 2), r.vn), (r.gctx.at[:, own_heads], r.gn)):
        in_order(base, out, spots, tok)
    for start in reversed(range(0, length, bq)):
        if poll:
            poll(start // bq)
        end = start + bq
        q, g = r.qn[start:end, :], r.gn[start:end, :]
        p = softmax_block(q, r.kn[:end, :], start, scale)
        dp = nt(g, r.vn[:end, :])
        ds = (p * (dp - jnp.sum(p * dp, -1, keepdims=True))).astype(BF16)
        gq_here = (nn(ds, r.kn[:end, :]) * scale).astype(BF16)
        for i in range(bq // tok):
            at = spots[start // tok + i]
            gq[at : at + tok, :] = gq_here[i * tok : (i + 1) * tok]
        dk, dv = tn(ds, q), tn(p.astype(BF16), g)
        if end == length:
            r.ks[...] = dk
            r.vs[...] = dv
        else:
            r.ks[:end, :] += dk
            r.vs[:end, :] += dv
    for b, at in enumerate(spots):
        here = slice(b * tok, (b + 1) * tok)
        gk[at : at + tok, :] = (r.ks[here, :] * scale).astype(BF16)
        gv[at : at + tok, :] = r.vs[here, :].astype(BF16)
    for i, ref in enumerate((gq, gk, gv)):
        r.late[0, i * rank : (i + 1) * rank, own_heads] = tn(r.lq[:, i * rank : (i + 1) * rank], ref[...]).astype(BF16)


def add_up_body(unit, r):
    e = pl.program_id(0)
    seqs, devs = r.early.shape[1], 2 * r.early.shape[2]
    d, ff = r.ino.shape[2], r.outu.shape[2]
    dl, fl, hd = d // devs, ff // devs, d // H
    for ref in (r.inq, r.outq, r.ino, r.outo, r.inu, r.outu, r.ind, r.outd):
        ref[...] = jnp.zeros_like(ref)

    @pl.loop(0, seqs)
    def _(q):
        @pl.when(r.index[q] == e)
        def _():
            for dev in range(devs):

                def add(ref, at, width, source, k, start, dev=dev):
                    ref[0, :, at : at + width] += source[dev % 2, q, dev // 2, k, :, start : start + width].astype(F32)

                for i in range(fl // unit):
                    add(r.outu, (i * devs + dev) * unit, unit, r.early, 0, i * unit)
                    add(r.ind, (i * devs + dev) * unit, unit, r.early, 1, i * unit)
                for i in range(dl // hd):
                    add(r.ino, (i * devs + dev) * hd, hd, r.middle, 0, i * hd)
                    add(r.outq, (i * devs + dev) * hd, hd, r.late, 0, i * hd)
                for i, ref in enumerate((r.inu, r.outo, r.outd)):
                    add(ref, dev * dl, dl, r.middle, 1 + i, 0)
                add(r.inq, dev * dl, dl, r.late, 1, 0)


def shards(
    inputs,
    norm_gain,
    norm_bias,
    w_qkv,
    qv_bias,
    w_out,
    out_bias,
    w_up,
    up_bias,
    w_down,
    down_bias,
    adapter_index,
    ad_in_qkv,
    ad_out_qkv,
    ad_in_out,
    ad_out_out,
    ad_in_up,
    ad_out_up,
    ad_in_down,
    ad_out_down,
    cotangent,
):
    y, c, z, x = (lax.axis_index(a) for a in ("y", "c", "z", "x"))
    ny, n, nx = lax.axis_size("y"), lax.axis_size("z"), lax.axis_size("x")
    group = 2 * nx
    mb, tok, d = inputs.shape[1:]
    rank = ad_out_out.shape[1]
    na = ad_in_qkv.shape[0]
    hd = d // H
    heads = H // group
    dl = d // group
    ff = up_bias.shape[0]
    fl = ff // group
    unit = fl // n
    seqs = adapter_index.shape[0]
    length = 2 * ny * mb * n * nx * tok // seqs
    zb = length // tok // nx
    per = n // zb
    own = length // group
    scale = hd**-0.5
    dev = x * 2 + c
    fast = nx == 2 and n == 4 and ny == 2
    assert zb == 4 and n == 2 * mb * per and mb == 2 and own == 2 * tok
    plan = (n, zb, per, mb)

    def half_at(v, axis, index):
        return lax.dynamic_index_in_dim(v, index, axis, keepdims=False)

    def part(v, shape, lead):
        v = v.reshape(v.shape[:lead] + shape + v.shape[lead + 1 :])
        v = half_at(v, lead + 1, x)
        return half_at(v, lead + 1, c)

    ff_shape, head_shape = (n, nx, 2, unit), (heads, nx, 2, hd)

    chosen = lax.dynamic_slice_in_dim(adapter_index, y * n + z, 1, 0)
    gains, shifts = norm_gain.astype(F32), norm_bias.astype(F32)
    outb, downb = out_bias[None], down_bias[None]
    tables = [
        jnp.swapaxes(ad_in_qkv, 1, 2),
        ad_out_qkv,
        jnp.swapaxes(ad_in_out, 1, 2),
        ad_out_out,
        jnp.swapaxes(ad_in_up, 1, 2),
        ad_out_up,
        jnp.swapaxes(ad_in_down, 1, 2),
        ad_out_down,
    ]

    def chosen_one(v):
        return pl.BlockSpec((1,) + v.shape[1:], lambda i, at: (at[0],) + (0,) * (v.ndim - 1))

    def flat_spec(shape):
        return pl.BlockSpec(shape, lambda i, at: (0,) * len(shape))

    picked = [
        sds((3 * rank, d)),
        sds((3 * rank, 3 * dl)),
        sds((group, rank, dl)),
        sds((rank, dl)),
        sds((rank, d)),
        sds((rank, d)),
        sds((rank, fl)),
        sds((rank, fl)),
        sds((rank, d)),
        sds((1, 3 * dl), F32),
        sds((1, fl), F32),
    ]
    biases = [qv_bias, up_bias[None]]
    in_qkv, ao, in_all, in_out, out_out, in_up, out_up, in_down, out_down, qkv_bias, upb = pl.pallas_call(
        functools.partial(select_body, group, heads, n, lambda: lax.axis_index("x") * 2 + lax.axis_index("c")),
        grid_spec=pltpu.PrefetchScalarGridSpec(
            num_scalar_prefetch=1,
            grid=(1,),
            in_specs=[chosen_one(t) for t in tables] + [flat_spec(b.shape) for b in biases],
            out_specs=[flat_spec(p.shape) for p in picked],
        ),
        out_shape=picked,
        name="select",
    )(chosen, *tables, *biases)

    row2 = (2, tok, d)
    blocks = (group, 2, tok, d)
    vec = full((1, d))

    def slow_deal(v):
        v = lax.all_gather(v[0], ("c", "z"))
        cs, h, m = z // (per * mb), z % per, (z // per) % mb
        return jnp.stack([half_at(half_at(v, 0, cs * n + h * zb + 2 * c + p), 0, m) for p in range(2)])

    def slow_undeal(v):
        v = lax.all_gather(v.reshape(row2), ("c", "z"))
        h, zz = z // zb, z % zb
        at = [(zz // 2) * n + (c * mb + m) * per + h for m in range(mb)]
        return jnp.stack([half_at(half_at(v, 0, a), 0, zz % 2) for a in at])[None]

    def slow_spread(v):
        return lax.all_gather(v.reshape(own, d), ("c", "x"), tiled=True)

    def slow_sum(v):
        return lax.psum_scatter(v.astype(F32), ("c", "x"), scatter_dimension=0, tiled=True)

    if not fast:
        xs, gs = slow_deal(inputs), slow_deal(cotangent)
        nh, _ = centre(xs.astype(F32))
        h1 = slow_spread((nh * gains[0] + shifts[0]).astype(BF16))
        wq = lax.all_gather(w_qkv, ("z", "x"), axis=1, tiled=True)
        wq = part(wq.reshape(d, 3, d), head_shape, 2).reshape(1, d, 3 * dl)

        def across(w, shape):
            w = half_at(w.reshape(shape + w.shape[1:]), 2, c)
            w = jnp.moveaxis(w, 1, 0).reshape(nx, -1, w.shape[-1])
            w = lax.all_to_all(w, "x", 0, 0)
            w = jnp.moveaxis(w, 0, 1).reshape(w.shape[1], -1)
            return lax.all_gather(w, "z")

        wo, wd = across(w_out, head_shape), across(w_down, ff_shape)
        wu = lax.all_gather(half_at(w_up.reshape(d, 2, -1), 1, c), "z")

    def carried(**arrays):
        ins = {k + "_in": (v, ANY) for k, v in arrays.items()}
        outs = {k: (sds(v.shape), ANY) for k, v in arrays.items()}
        return ins, outs, [(k + "_in", k) for k in arrays]

    if not fast:
        np_, _, nq = wq.shape
        qkv_ins = dict(
            h=(h1, once((length, d))),
            w=(wq, pl.BlockSpec((1, d, nq), lambda i: (i, 0, 0))),
            low_in=(in_qkv, full((3 * rank, d))),
            low_out=(ao, cols(3 * rank, nq)),
            bias=(qkv_bias, cols(1, nq)),
        )
        qkv_outs = dict(out=(sds((length, 3 * dl)), cols(length, nq)), lq=(sds((length, 3 * rank)), full((length, 3 * rank))))
        k1 = run(qkv_body, qkv_ins, qkv_outs, "qkv", (np_,))
        qkv, lq = k1.out, k1.lq

    bq = 256
    spots = places(length, tok, nx)
    setup = (bq, tok, spots, scale)

    def head_cols(base):
        return pl.BlockSpec((length, hd), lambda i: (0, base + i))

    def head_scratch(names):
        return {k: pltpu.VMEM((length, hd), BF16) for k in names}

    att_outs = dict(ctx=(sds((length, dl)), head_cols(0)))
    att_flops = 2 * heads * length * length * hd

    def att_ins():
        return dict(q=(qkv, head_cols(0)), k=(qkv, head_cols(heads)), v=(qkv, head_cols(2 * heads)))

    if not fast:
        k2 = run(functools.partial(attend_body, *setup), att_ins(), att_outs, "attend", (heads,), head_scratch(("qn", "kn", "vn")))
        g, ctx = slow_spread(gs), k2.ctx

    def sum_scratch(a, w, more):
        return dict(
            av=pltpu.VMEM(a.shape, BF16),
            wv=pltpu.VMEM(w.shape, BF16),
            part=pltpu.VMEM((4, own, d), BF16),
            got=pltpu.VMEM((4, own, d), BF16),
            ls=pltpu.SemaphoreType.DMA((16,)),
            lh=pltpu.SemaphoreType.DMA((2,)),
            **more,
        )

    def low_scratch(rows):
        return dict(low1=pltpu.VMEM((2, rows, length), BF16), low2=pltpu.VMEM((2, rows, length), BF16))

    def group_low(a, low):
        return lax.psum(jnp.dot(a, low.T, preferred_element_type=F32), ("c", "x")).astype(BF16)

    def slow_product(block, a, w, name):
        out = run(
            functools.partial(plain_product_body, block),
            dict(a=(a, WHOLE), w=(w, WHOLE)),
            dict(out=(sds((length, d)), WHOLE)),
            name,
        ).out
        return slow_sum(out)

    def mine(v):
        return lax.dynamic_slice_in_dim(v, (c * nx + x) * own, own, 0)

    def quarter(v):
        return lax.dynamic_slice_in_dim(v, dev * dl, dl, 1)

    def slow_term(low, v):
        return lax.dot_general(low, v, (((0,), (0,)), ((), ())), preferred_element_type=F32).astype(BF16)

    def dot(a, b):
        return jnp.dot(a, b, preferred_element_type=F32)

    if fast:
        four = pltpu.SemaphoreType.DMA((4,))
        wide = 2 * n
        k3 = run(
            functools.partial(front_body, *plan, setup),
            {
                "inputs": (inputs, ANY),
                "cot": (cotangent, ANY),
                "wq_in": (w_qkv.reshape(2, 2, d // 4, -1), ANY),
                "wo_in": (w_out.reshape(2, heads // 2, 2, 2, hd, -1), ANY),
                "wu_in": (w_up.reshape(2, 2, d // 4, -1), ANY),
                "wd_in": (w_down.reshape(2, n // 2, 2, 2, unit, -1), ANY),
                "low_in": (in_qkv, WHOLE),
                "low_out": (ao, WHOLE),
                "bias": (qkv_bias, WHOLE),
                "low": (in_out, WHOLE),
                "bias2": (outb, WHOLE),
                "low_out2": (out_out, WHOLE),
                "gain": (norm_gain, WHOLE),
                "shift": (norm_bias, WHOLE),
            },
            {
                "wq": (sds((n, 2, 2, d // 4, 3 * hd)), ANY),
                "wo": (sds((n, 2, heads // 2, hd, d // n)), ANY),
                "wu": (sds((n, 2, 2, d // 4, unit)), ANY),
                "wd": (sds((n, 2, n // 2, unit, d // n)), ANY),
                "h1": (sds(blocks), ANY),
                "x": (sds(row2), WHOLE),
                "gs": (sds(row2), WHOLE),
                "qkv": (sds((length, 3 * dl)), WHOLE),
                "lq": (sds((length, 3 * rank)), WHOLE),
                "ctx": (sds((length, dl)), WHOLE),
                "mid": (sds(row2, F32), WHOLE),
                "h": (sds(blocks), ANY),
                "lows": (sds((rank, length)), WHOLE),
                "wof": (sds((group, n, 2, heads // 2, hd, d // n)), ANY),
            },
            "front",
            scratch={
                **head_scratch(("qn", "kn", "vn")),
                "xv": pltpu.VMEM(row2, BF16),
                "gv": pltpu.VMEM(row2, BF16),
                "hv": pltpu.VMEM(row2, BF16),
                "hv2": pltpu.VMEM(row2, BF16),
                "qs": pltpu.VMEM((2, 2, d // 4, 2 * hd), BF16),
                "os": pltpu.VMEM((2, heads // 2, hd, d // wide), BF16),
                "us": pltpu.VMEM((2, 2, d // 4, unit), BF16),
                "ds": pltpu.VMEM((2, n // 2, unit, d // wide), BF16),
                "h1v": pltpu.VMEM(blocks, BF16),
                "wqv": pltpu.VMEM((n, 2, 2, d // 4, 3 * hd), BF16),
                "wv": pltpu.VMEM((n, 2, heads // 2, hd, d // n), BF16),
                "part": pltpu.VMEM((4, own, d), BF16),
                "got": pltpu.VMEM((4, own, d), BF16),
                "lowv": pltpu.VMEM((tok, d), F32),
                "ls": pltpu.SemaphoreType.DMA((5,)),
                "ls8": pltpu.SemaphoreType.DMA((8,)),
                "lh": pltpu.SemaphoreType.DMA((2,)),
                "lh1": pltpu.SemaphoreType.DMA((2,)),
                "lhw": four,
                "lq1": four,
                "lq2": four,
                "dsend": four,
                "drecv": four,
                **low_scratch(rank),
                **links_scratch(108),
            },
            cid=0,
            flops=2 * length * d * (3 * dl + dl) + 2 * att_flops,
        )
        xs, gs, qkv, lq, ctx = k3.x, k3.gs, k3.qkv, k3.lq, k3.ctx
        wq, wo, h1 = k3.wq.reshape(n, d, 3 * hd), k3.wo.reshape(n, dl, d // n), k3.h1.reshape(length, d)
        mid, h2, low_rows, wu, wd = k3.mid, k3.h.reshape(length, d), k3.lows, k3.wu, k3.wd
    else:
        lo = group_low(ctx, in_out)
        low_rows = lo.T
        mid = xs.reshape(own, d).astype(F32) + slow_product(forward_block, ctx, wo, "attn_out") + outb + dot(mine(lo), out_out)
        nh, _ = centre(mid)
        h2 = slow_spread((nh * gains[1] + shifts[1]).astype(BF16))
        mid = mid.reshape(row2)

    def flat(w):
        return w.reshape(n, -1, w.shape[-1])

    if fast:
        ins, outs, alias = carried(wd=wd)
        k5 = run(
            functools.partial(up_body_fast, n),
            {
                "h": (h2, ANY),
                "wu": (flat(wu), ANY),
                "low_in": (in_up, WHOLE),
                "low_out": (out_up, WHOLE),
                "bias": (upb, WHOLE),
                "gs": (gs, WHOLE),
                "low_out2": (out_down, WHOLE),
                "low_in2": (in_down, WHOLE),
                **ins,
            },
            {
                "act": (sds((length, fl // 2)), ANY),
                "gpre": (sds((length, fl // 2)), ANY),
                "acc1": (sds((length, d), F32), ANY),
                "acc2": (sds((length, d), F32), ANY),
                "glu_part": (sds((rank, length)), WHOLE),
                "ld_part": (sds((rank, length)), WHOLE),
                "terms": (sds((2, rank, fl)), WHOLE),
                "g4": (sds(blocks), ANY),
                **outs,
            },
            "up",
            scratch={
                "hv": pltpu.VMEM((length, d), BF16),
                "gv": pltpu.VMEM(blocks, BF16),
                "lsp": pltpu.SemaphoreType.DMA((2,)),
                "wuv": pltpu.VMEM((n, d, unit), BF16),
                "wdv": pltpu.VMEM((2, 2, n, unit, d // n), BF16),
                "stage": pltpu.VMEM((2, own, d), F32),
                "gluv": pltpu.VMEM((rank, length), F32),
                "ldv": pltpu.VMEM((rank, length), F32),
                "lk1": pltpu.SemaphoreType.DMA((2,)),
                "lk2": pltpu.SemaphoreType.DMA((2,)),
                "actv": pltpu.VMEM((length, fl), BF16),
                "slopev": pltpu.VMEM((length, fl), BF16),
                "gprev": pltpu.VMEM((length, fl), BF16),
                "lu": pltpu.VMEM((length, rank), BF16),
                "gld": pltpu.VMEM((length, rank), BF16),
                "lh": four,
                "lg": four,
                "lu1": four,
                "lo1": four,
                "lo2": four,
                "lw": four,
                **links_scratch(24),
            },
            alias=alias,
            cid=4,
            flops=4 * length * d * fl,
        )
        act, wu, wd, g = k5.act, flat(wu), flat(k5.wd), k5.g4.reshape(length, d)
    else:
        up_ins = dict(
            h=(h2, once((length, d))),
            w=(flat(wu), pl.BlockSpec((1, d, unit), lambda i: (i, 0, 0))),
            low_in=(in_up, full((rank, d))),
            low_out=(out_up, cols(rank, unit)),
            bias=(upb, cols(1, unit)),
        )
        up_outs = dict(
            act=(sds((length, fl)), cols(length, unit)),
            slope=(sds((length, fl)), cols(length, unit)),
            lu=(sds((length, rank)), full((length, rank))),
        )
        k4 = run(up_body, up_ins, up_outs, "up", (n,))
        act, slope, lu = k4.act, k4.slope, k4.lu

        ft = min(512, fl)
        k5 = run(
            gpre_body,
            dict(
                g=(g, once((length, d))),
                w=(wd, pl.BlockSpec((n, ft, d // n), lambda i: (0, i, 0))),
                slope=(slope, cols(length, ft)),
                act=(act, cols(length, ft)),
                low_out=(out_down, full((rank, d))),
                low_in=(in_down, cols(rank, ft)),
                lu=(lu, full((length, rank))),
            ),
            dict(
                gpre=(sds((length, fl)), cols(length, ft)),
                gld=(sds((length, rank)), full((length, rank))),
                terms=(sds((2, rank, fl)), pl.BlockSpec((2, rank, ft), lambda i: (0, 0, i))),
            ),
            "gpre",
            (fl // ft,),
            flops=2 * length * d * fl,
        )
    gpre = k5.gpre

    def shared(v):
        return (2, ny, n, nx) + v.shape

    def slow_share(v):
        return lax.all_gather(v, ("c", "y", "z", "x")).reshape(shared(v))


    if fast:
        k6 = run(
            functools.partial(gmid_body, n),
            {
                "a": (gpre, ANY),
                "w": (wu.reshape(n // 2, 2, d, unit), ANY),
                "low": (k5.glu_part, WHOLE),
                "acc1": (k5.acc1, ANY),
                "b": (act, ANY),
                "v": (wd.reshape(n, n // 2, 2, unit, d // n), ANY),
                "low_b": (k5.ld_part, WHOLE),
                "acc2": (k5.acc2, ANY),
                "mid": (mid, WHOLE),
                "g": (gs, WHOLE),
                "low_in": (in_up, WHOLE),
                "gain": (norm_gain, WHOLE),
                "full": (h2, ANY),
                "full_b": (g, ANY),
                "pack": (k5.terms, WHOLE),
                "wof": (k3.wof.reshape(n, d, d // n), ANY),
                "out_out": (out_out, WHOLE),
                "in_all": (in_all, WHOLE),
                "lo": (low_rows, WHOLE),
            },
            {
                "gmid": (sds(row2, F32), WHOLE),
                "gctx": (sds((group, 2, tok, dl)), ANY),
                "glo": (sds((group, rank, own)), WHOLE),
                "lows": (sds((rank, length)), WHOLE),
                "terms": (sds((3, rank, dl)), WHOLE),
                "shared": (sds(shared(k5.terms)), ANY),
                "sb": (sds(row2), WHOLE),
                "sd": (sds(row2, F32), WHOLE),
            },
            "gmid",
            scratch={
                **sum_scratch(gpre, wu[: n // 2], dict(hv=pltpu.VMEM(row2, BF16), **low_scratch(rank))),
                "bv": pltpu.VMEM(act.shape, BF16),
                "vv": pltpu.VMEM((n, 2, unit, d // n), BF16),
                "wfv": pltpu.VMEM((n, d, d // n), BF16),
                "i1": pltpu.VMEM((length, d), F32),
                "li1": four,
                "li2": four,
                "part2": pltpu.VMEM((4, own, d), BF16),
                "got2": pltpu.VMEM((3, own, d), BF16),
                "low1b": pltpu.VMEM((2, rank, length), BF16),
                "low2b": pltpu.VMEM((2, rank, length), BF16),
                "glu": pltpu.VMEM((rank, length), BF16),
                "lowv": pltpu.VMEM((tok, d), F32),
                "fv": pltpu.VMEM((length, dl), BF16),
                "gv": pltpu.VMEM((length, dl), BF16),
                "send": pltpu.VMEM((2, group, tok, dl), BF16),
                "glos": pltpu.VMEM((group, rank, own), BF16),
                "tsend": pltpu.VMEM((group, rank, dl), BF16),
                "tgot": pltpu.VMEM((group, rank, dl), BF16),
                "lsh": pltpu.SemaphoreType.DMA((4,)),
                **links_scratch(40),
            },
            cid=5,
            flops=4 * length * d * fl,
        )
        gmid, before, early = k6.gmid, k6.terms, k6.shared
    else:
        glu = group_low(gpre, out_up)
        gh = slow_product(backward_block, gpre, wu, "gmid") + dot(mine(glu), in_up)
        gmid = gs.reshape(own, d).astype(F32) + norm_back(mid.reshape(own, d), gh, gains[1])
        gattn = slow_spread(gmid.astype(BF16))
        ld = group_low(act, in_down)
        out = mid.reshape(own, d) + slow_product(forward_block, act, wd, "outputs") + downb + dot(mine(ld), out_down)
        outputs = slow_undeal(out.astype(BF16))
        before = jnp.stack([slow_term(glu, quarter(h2)), slow_term(ld, quarter(g))])
        early = slow_share(k5.terms)

    ab_scratch = {
        **head_scratch(("qn", "kn", "vn", "gn")),
        "ks": pltpu.VMEM((length, hd), F32),
        "vs": pltpu.VMEM((length, hd), F32),
        "gctx": pltpu.VMEM((length, dl), BF16),
    }
    ab_ins = {"lq": (lq, WHOLE), "before": (before, WHOLE)}
    if fast:
        k9 = run(
            functools.partial(back_body, plan, setup),
            {
                **ab_ins,
                "sb": (k6.sb, ANY),
                "wq": (wq, ANY),
                "glo": (k6.glo, WHOLE),
                "gctx_in": (k6.gctx.reshape(length, dl), ANY),
                "ctx_in": (ctx, ANY),
                "qkv_in": (qkv, ANY),
                "mid_in": (mid, ANY),
                "sd_in": (k6.sd, ANY),
                "gmid_in": (gmid, ANY),
                "x_in": (xs, ANY),
                "full": (h1, ANY),
                "ao": (ao, WHOLE),
                "ld": (k6.lows, WHOLE),
                "low_down": (out_down, WHOLE),
                "low_back": (in_qkv, WHOLE),
                "bias": (downb, WHOLE),
                "gain": (norm_gain, WHOLE),
            },
            {
                "back": (sds(inputs.shape), ANY),
                "outputs": (sds(inputs.shape), ANY),
                "shared_m": (sds((2, ny, n, nx, 4, rank, dl)), ANY),
                "shared_l": (sds((2, ny, n, nx, 2, 3 * rank, dl)), ANY),
            },
            "back",
            scratch={
                **ab_scratch,
                **low_scratch(3 * rank),
                "ctx": pltpu.VMEM((length, dl), BF16),
                "qkv": pltpu.VMEM((length, 3 * dl), BF16),
                "out": pltpu.VMEM((length, 3 * dl), BF16),
                "wqv": pltpu.VMEM(wq.shape, BF16),
                "part": pltpu.VMEM((4, own, d), BF16),
                "got": pltpu.VMEM((4, own, d), BF16),
                "mid": pltpu.VMEM(row2, F32),
                "sd": pltpu.VMEM(row2, F32),
                "gmid": pltpu.VMEM(row2, F32),
                "x": pltpu.VMEM(row2, BF16),
                "rb": pltpu.VMEM(row2, BF16),
                "outv": pltpu.VMEM(row2, BF16),
                "gv": pltpu.VMEM(row2, BF16),
                "terms": pltpu.VMEM((4, rank, dl), BF16),
                "late": pltpu.VMEM((2, 3 * rank, dl), BF16),
                "fv": pltpu.VMEM((length, dl), BF16),
                "glq": pltpu.VMEM((3 * rank, length), BF16),
                "lowv": pltpu.VMEM((tok, d), F32),
                "lowb": pltpu.VMEM((2, tok, d), F32),
                "ls": pltpu.SemaphoreType.DMA((8,)),
                "ld8": pltpu.SemaphoreType.DMA((8,)),
                "lsh": pltpu.SemaphoreType.DMA((3,)),
                "dsend": pltpu.SemaphoreType.DMA((6,)),
                "drecv": pltpu.SemaphoreType.DMA((6,)),
                **links_scratch(36),
            },
            cid=6,
            flops=5 * att_flops // 2 + 2 * length * d * 4 * dl,
        )
        middle, late = k9.shared_m, k9.shared_l
        input_grad, outputs = k9.back.astype(F32), k9.outputs
    else:

        def attend_back_plain(r):
            pl.when(pl.program_id(0) == 0)(lambda: gctx_body(lambda: lax.axis_index("x") * 2 + lax.axis_index("c"), r))
            attend_back_body(*setup, r, pl.program_id(0), heads)

        k9 = run(
            attend_back_plain,
            {
                **ab_ins,
                "low_out": (out_out, WHOLE),
                "low_in": (in_out, WHOLE),
                "lo": (low_rows, WHOLE),
                "qkv": (qkv, WHOLE),
                "ga": (gattn, WHOLE),
                "w": (wo, WHOLE),
                "ctx": (ctx, WHOLE),
            },
            dict(
                out=(sds((length, 3 * dl)), WHOLE),
                late=(sds((2, 3 * rank, dl)), WHOLE),
                terms=(sds((4, rank, dl)), WHOLE),
            ),
            "attend_back",
            (heads,),
            {**ab_scratch, "glo": pltpu.VMEM((length, rank), BF16)},
        )
        glq = group_low(k9.out, ao)
        middle = slow_share(k9.terms)
        late = slow_share(jnp.stack([k9.late[0], slow_term(glq, quarter(h1))]))
        gh = slow_product(backward_block, k9.out, wq, "input_grad") + dot(mine(glq), in_qkv)
        gx = gmid + norm_back(xs.reshape(own, d).astype(F32), gh, gains[0])
        input_grad = slow_undeal(gx.astype(BF16)).astype(F32)

    def by_seq(v):
        return v.reshape((2, seqs, nx) + v.shape[4:])

    def one(height, width):
        return sds((na, height, width), F32), pl.BlockSpec((1, height, width), lambda e: (e, 0, 0))

    k11 = run(
        functools.partial(add_up_body, unit),
        dict(
            index=(adapter_index, pl.BlockSpec(memory_space=pltpu.SMEM)),
            early=(by_seq(early), WHOLE),
            middle=(by_seq(middle), WHOLE),
            late=(by_seq(late), WHOLE),
        ),
        dict(
            inq=one(3 * rank, d),
            outq=one(3 * rank, d),
            ino=one(rank, d),
            outo=one(rank, d),
            inu=one(rank, d),
            outu=one(rank, ff),
            ind=one(rank, ff),
            outd=one(rank, d),
        ),
        "add_up",
        (na,),
    )

    def turn(v):
        return jnp.swapaxes(v, 1, 2)

    return (
        outputs,
        input_grad,
        turn(k11.inq),
        k11.outq.reshape(na, 3, rank, d),
        turn(k11.ino),
        k11.outo,
        turn(k11.inu),
        k11.outu,
        turn(k11.ind),
        k11.outd,
    )


def solution(mesh):
    act = P(("y", "c"), None, ("z", "x"), None)
    weight = P(None, ("z", "x"))
    ins = (act, P(), P(), weight, P(), weight, P(), weight, P(), weight) + (P(),) * 10 + (act,)

    def program(*arrays):
        ndp, nf = mesh.devices.shape
        ny = ndp // 2
        n = arrays[11].shape[0] // ny
        grid = Mesh(mesh.devices.reshape(ny, 2, n, nf // n), ("y", "c", "z", "x"))
        return jax.shard_map(
            shards,
            mesh=grid,
            in_specs=ins,
            out_specs=(act, act) + (P(),) * 8,
            check_vma=False,
        )(*arrays)

    return program
```
